64 devices in a mesh: dp: 4 (over x, y), ep: 16 (over z, core).
Axes of the slice: x: 2, y: 2, z: 8, core: 2. Of those that a mesh axis runs over, the one named last changes fastest.
The devices are a block of a 4x4x8 slice.
Arguments:
- hidden: bfloat16 [16384, 1024], P(('dp', 'ep')), parts along dimension 0
- w_gate: bfloat16 [32, 1024, 512], P('ep')
- w_up: bfloat16 [32, 1024, 512], P('ep')
- w_down: bfloat16 [32, 512, 1024], P('ep')
- w_router: bfloat16 [1024, 32], replicated
- slot_expert: int32 [192], P('dp'), parts along dimension 0
- topk_idx: int32 [16384, 8], P(('dp', 'ep')), parts along dimension 0
- topk_slot: int32 [16384, 8], P(('dp', 'ep')), parts along dimension 0
Outputs:
- output 1: bfloat16 [16384, 1024], P(('dp', 'ep')), parts along dimension 0
- output 2: bfloat16 [192, 1024, 512], P(('dp', 'ep')), parts along dimension 0
- output 3: bfloat16 [192, 1024, 512], P(('dp', 'ep')), parts along dimension 0
- output 4: bfloat16 [192, 512, 1024], P(('dp', 'ep')), parts along dimension 0
There are 4 independent parts. The reference program is written for one: setup_inputs(seed, part) draws one part's arguments, and reference() takes and returns one part's arrays. A program takes and returns all parts, laid end to end along the dimension named above; an argument that names none is the same for every part.
All inputs are finite; a program needn't handle non-finite values.
Results may differ from the reference program's by a relative error of at most 0.00789102.
Values are sent between devices in bfloat16 or wider.
A program may use at most 768 MiB of HBM per device.

```python
import jax
import jax.numpy as jnp
from jax import lax

HIDDEN = 1024
INTER = 512
EXPERTS = 32
TOP = 8
GROUP = 16
TOKENS_DEV = 256

SLOTS = EXPERTS + GROUP
SLOTS_DEV = SLOTS // GROUP
LOCAL_EXP = EXPERTS // GROUP
TOKENS = GROUP * TOKENS_DEV
PAIRS = TOKENS * TOP
HOT_COUNT = GROUP // 2
HOT_SLOTS = 3 * HOT_COUNT
CAP = 2 * PAIRS // (SLOTS + HOT_SLOTS)
ROUTE_SCALE = 5.0 / 2.0


def draw_routing(route_key):
    k_hot, k_move, k_perm, k_shift, k_rows = jax.random.split(route_key, 5)
    slot_ids = jnp.arange(SLOTS)
    hot_experts = jax.random.permutation(k_hot, EXPERTS)[:HOT_COUNT]
    dev_of_slot = slot_ids // SLOTS_DEV
    pos_in_dev = slot_ids % SLOTS_DEV
    base_table = jnp.where(pos_in_dev < LOCAL_EXP, dev_of_slot * LOCAL_EXP + pos_in_dev, hot_experts[dev_of_slot // 2])
    moving = jax.random.randint(k_move, (SLOTS,), 0, 4) > 0
    dest_pos = jnp.argsort(jnp.where(moving, 0, 1) * SLOTS + slot_ids)
    scores = jax.random.randint(k_perm, (SLOTS,), 0, SLOTS)
    src_pos = jnp.argsort(jnp.where(moving, scores, SLOTS) * SLOTS + slot_ids)
    slot_expert = base_table.at[dest_pos].set(base_table[src_pos])
    is_hot = jnp.zeros((EXPERTS,), jnp.int32).at[hot_experts].set(1)
    slot_hot = is_hot[slot_expert]
    cold_count = SLOTS - HOT_SLOTS
    rest_pairs = PAIRS - CAP * HOT_SLOTS
    cold_rank = jnp.cumsum(1 - slot_hot) - 1
    shift_by = jax.random.randint(k_shift, (), 0, cold_count)
    extra_one = ((cold_rank + shift_by) % cold_count < rest_pairs % cold_count).astype(jnp.int32)
    slot_loads = jnp.where(slot_hot > 0, CAP, rest_pairs // cold_count + extra_one)
    slot_order = jnp.argsort(slot_expert * SLOTS + slot_ids)
    pair_slot = jnp.repeat(slot_order, slot_loads[slot_order], total_repeat_length=PAIRS)
    pair_table = pair_slot.reshape(TOP, TOKENS).T
    row_perm = jax.random.permutation(k_rows, TOKENS)
    topk_slot = pair_table[row_perm]
    topk_idx = slot_expert[topk_slot]
    return slot_expert, topk_idx, topk_slot


def setup_inputs(seed: int = 0, part: int = 0) -> dict:
    base_key = jax.random.key(seed)
    k_shared, k_local = jax.random.split(base_key)
    k_local = jax.random.fold_in(k_local, part)
    k_gate, k_up, k_down, k_router = jax.random.split(k_shared, 4)
    k_hidden, k_route = jax.random.split(k_local)
    hidden = jax.random.normal(k_hidden, (TOKENS, HIDDEN), jnp.float32).astype(jnp.bfloat16)
    w_gate = (jax.random.normal(k_gate, (EXPERTS, HIDDEN, INTER), jnp.float32) * HIDDEN ** -0.5).astype(jnp.bfloat16)
    w_up = (jax.random.normal(k_up, (EXPERTS, HIDDEN, INTER), jnp.float32) * HIDDEN ** -0.5).astype(jnp.bfloat16)
    w_down = (jax.random.normal(k_down, (EXPERTS, INTER, HIDDEN), jnp.float32) * INTER ** -0.5).astype(jnp.bfloat16)
    w_router = (jax.random.normal(k_router, (HIDDEN, EXPERTS), jnp.float32) * 2.0 * HIDDEN ** -0.5).astype(jnp.bfloat16)
    slot_expert, topk_idx, topk_slot = draw_routing(k_route)
    return {"hidden": hidden, "w_gate": w_gate, "w_up": w_up, "w_down": w_down, "w_router": w_router, "slot_expert": slot_expert, "topk_idx": topk_idx, "topk_slot": topk_slot}


def reference(hidden, w_gate, w_up, w_down, w_router, slot_expert, topk_idx, topk_slot):
    p_gate = jnp.take(w_gate, slot_expert, axis=0)
    p_up = jnp.take(w_up, slot_expert, axis=0)
    p_down = jnp.take(w_down, slot_expert, axis=0)
    logits = jnp.dot(hidden, w_router, preferred_element_type=jnp.float32)
    chosen = jax.nn.sigmoid(jnp.take_along_axis(logits, topk_idx, axis=1))
    gates = ROUTE_SCALE * chosen / jnp.sum(chosen, axis=1, keepdims=True)
    flat_slot = topk_slot.reshape(PAIRS)
    flat_gate = gates.reshape(PAIRS)
    sorted_pairs = jnp.argsort(flat_slot * PAIRS + jnp.arange(PAIRS))
    counts = jax.ops.segment_sum(jnp.ones((PAIRS,), jnp.int32), flat_slot, num_segments=SLOTS)
    starts = jnp.cumsum(counts) - counts
    slot_rank = jnp.arange(CAP)

    def one_slot(acc_rows, slot_id):
        picked = sorted_pairs[jnp.minimum(starts[slot_id] + slot_rank, PAIRS - 1)]
        pair_weight = jnp.where(slot_rank < counts[slot_id], flat_gate[picked], 0.0)
        tok_ids = picked // TOP
        rows_in = hidden[tok_ids]
        act_a = jnp.dot(rows_in, p_gate[slot_id], preferred_element_type=jnp.float32)
        act_b = jnp.dot(rows_in, p_up[slot_id], preferred_element_type=jnp.float32)
        hidden_act = (jax.nn.silu(act_a) * act_b).astype(jnp.bfloat16)
        expert_out = jnp.dot(hidden_act, p_down[slot_id], preferred_element_type=jnp.float32).astype(jnp.bfloat16)
        acc_rows = acc_rows.at[tok_ids].add(pair_weight[:, None] * expert_out.astype(jnp.float32))
        return acc_rows, None

    y_sum, _ = lax.scan(one_slot, jnp.zeros((TOKENS, HIDDEN), jnp.float32), jnp.arange(SLOTS))
    return y_sum.astype(jnp.bfloat16), p_gate, p_up, p_down
```

```python
import functools

import jax
import jax.numpy as jnp
from jax import lax
from jax.experimental import pallas as pl
from jax.experimental.pallas import tpu as pltpu
from jax.sharding import PartitionSpec as P

ROUTE_SCALE = 2.5
LANES = 128
TILE = 512


def experts_kernel(first_ref, x_ref, router_ref, gate_ref, up_ref, down_ref, out_ref):
    width = router_ref.shape[0]
    rows = x_ref[:, :width]
    chosen = x_ref[:, width:].astype(jnp.float32) > 0.5
    logits = jnp.dot(rows, router_ref[...], preferred_element_type=jnp.float32)
    gates = jnp.where(chosen, jax.nn.sigmoid(logits), 0.0)
    weights = ROUTE_SCALE * gates / jnp.sum(gates, axis=1, keepdims=True)
    lane = lax.broadcasted_iota(jnp.int32, weights.shape, 1)
    for i in range(gate_ref.shape[0]):
        mine = (lane == first_ref[0] + i) & chosen
        weight = jnp.sum(jnp.where(mine, weights, 0.0), axis=1, keepdims=True)
        served = jnp.sum(jnp.where(mine, 1.0, 0.0), axis=1, keepdims=True) > 0.5
        act_a = jnp.dot(rows, gate_ref[i], preferred_element_type=jnp.float32)
        act_b = jnp.dot(rows, up_ref[i], preferred_element_type=jnp.float32)
        hidden_act = (jax.nn.silu(act_a) * act_b).astype(jnp.bfloat16)
        expert_out = jnp.dot(hidden_act, down_ref[i], preferred_element_type=jnp.float32)
        contrib = jnp.where(served, weight * expert_out.astype(jnp.bfloat16).astype(jnp.float32), 0.0)
        if i == 0:
            out_ref[...] = contrib
        else:
            out_ref[...] += contrib


def apply_experts(first, tokens, router, w_gate, w_up, w_down):
    num_tokens, ext_width = tokens.shape
    experts, width, inter = w_gate.shape
    whole = lambda shape: pl.BlockSpec(shape, lambda t, *_: (0,) * len(shape))
    return pl.pallas_call(
        experts_kernel,
        grid_spec=pltpu.PrefetchScalarGridSpec(
            num_scalar_prefetch=1,
            grid=(num_tokens // TILE,),
            in_specs=[
                pl.BlockSpec((TILE, ext_width), lambda t, *_: (t, 0)),
                whole(router.shape), whole(w_gate.shape), whole(w_up.shape), whole(w_down.shape),
            ],
            out_specs=pl.BlockSpec((TILE, width), lambda t, *_: (t, 0)),
        ),
        out_shape=jax.ShapeDtypeStruct((num_tokens, width), jnp.float32),
        compiler_params=pltpu.CompilerParams(vmem_limit_bytes=48 * 1024 * 1024),
        cost_estimate=pl.CostEstimate(flops=6 * num_tokens * experts * width * inter, bytes_accessed=40 * 2**20, transcendentals=0),
        name="experts",
    )(first, tokens, router, w_gate, w_up, w_down)


def pick_kernel(table_ref, in_ref, out_ref):
    out_ref[...] = in_ref[...]


def pick_pieces(table, pieces):
    count = table.shape[0]
    block = (1,) + pieces.shape[1:]
    return pl.pallas_call(
        pick_kernel,
        grid_spec=pltpu.PrefetchScalarGridSpec(
            num_scalar_prefetch=1,
            grid=(count,),
            in_specs=[pl.BlockSpec(block, lambda i, table: (table[i], 0, 0))],
            out_specs=pl.BlockSpec(block, lambda i, table: (i, 0, 0)),
        ),
        out_shape=jax.ShapeDtypeStruct((count,) + pieces.shape[1:], pieces.dtype),
        name="pick",
    )(table, pieces)


def exchange_kernel(groups, picked_ref, out_ref, stage, local_sem, send_sem, recv_sem):
    me = lax.axis_index("dp")
    ep = lax.axis_index("ep")
    rows = picked_ref.shape[2]
    barrier = pltpu.get_barrier_semaphore()
    for k in range(1, groups):
        pl.semaphore_signal(barrier, inc=1, device_id=(lax.rem(me + k, groups), ep), device_id_type=pl.DeviceIdType.MESH)
    pl.semaphore_wait(barrier, groups - 1)
    place = pl.ds(pl.multiple_of(me * rows, rows), rows)
    copies = []
    for k in range(1, groups):
        peer = lax.rem(me + k, groups)
        copy = pltpu.make_async_remote_copy(
            src_ref=picked_ref.at[peer],
            dst_ref=out_ref.at[:, place, :],
            send_sem=send_sem.at[k],
            recv_sem=recv_sem.at[k],
            device_id=(peer, ep),
            device_id_type=pl.DeviceIdType.MESH,
        )
        copy.start()
        copies.append(copy)
    load = pltpu.make_async_copy(picked_ref.at[me], stage, local_sem.at[0])
    load.start()
    load.wait()
    store = pltpu.make_async_copy(stage, out_ref.at[:, place, :], local_sem.at[1])
    store.start()
    store.wait()
    for copy in copies:
        copy.wait()


def exchange(picked, groups, which):
    _, slots, rows, columns = picked.shape
    return pl.pallas_call(
        functools.partial(exchange_kernel, groups),
        out_shape=jax.ShapeDtypeStruct((slots, rows * groups, columns), picked.dtype),
        in_specs=[pl.BlockSpec(memory_space=pl.ANY)],
        out_specs=pl.BlockSpec(memory_space=pl.ANY),
        scratch_shapes=[
            pltpu.VMEM((slots, rows, columns), picked.dtype),
            pltpu.SemaphoreType.DMA((2,)),
            pltpu.SemaphoreType.DMA((groups,)),
            pltpu.SemaphoreType.DMA((groups,)),
        ],
        compiler_params=pltpu.CompilerParams(collective_id=which, has_side_effects=True),
        cost_estimate=pl.CostEstimate(flops=10**9, bytes_accessed=9 * 2**20, transcendentals=0),
        name="exchange",
    )(picked)


def solution(mesh):
    members = mesh.shape["ep"]
    groups = mesh.shape["dp"]
    tok_spec = P(("dp", "ep"), None)
    weight_spec = P("ep", None, None)
    slot_spec = P(("dp", "ep"), None, None)

    def local_block(hid_rows, w_gate, w_up, w_down, w_router, slot_expert, topk_idx, topk_slot):
        dp_index = lax.axis_index("dp")
        ep_index = lax.axis_index("ep")
        width, experts = w_router.shape
        per_dev = slot_expert.shape[0] // members

        chosen = jnp.any(topk_idx[:, :, None] == jnp.arange(LANES)[None, None, :], axis=1).astype(hid_rows.dtype)
        tokens = lax.all_gather(jnp.concatenate([hid_rows, chosen], axis=1), "ep", tiled=True)
        router = jnp.pad(w_router, ((0, 0), (0, LANES - experts)))
        first = (ep_index * w_gate.shape[0]).astype(jnp.int32).reshape(1)
        partial = apply_experts(first, tokens, router, w_gate, w_up, w_down)
        y_rows = lax.psum_scatter(partial, "ep", scatter_dimension=0, tiled=True)

        my_slots = lax.dynamic_slice_in_dim(slot_expert, ep_index * per_dev, per_dev)
        table = lax.all_gather(my_slots, "dp", tiled=True)

        def place(weight, which):
            rows = weight.shape[1] // groups
            piece = lax.dynamic_slice_in_dim(weight, dp_index * rows, rows, axis=1)
            pieces = lax.all_gather(piece, "ep", tiled=True)
            picked = pick_pieces(table, pieces).reshape(groups, per_dev, rows, weight.shape[2])
            return exchange(picked, groups, which)

        p_gate, p_up, p_down = place(w_gate, 0), place(w_up, 1), place(w_down, 2)
        return y_rows.astype(jnp.bfloat16), p_gate, p_up, p_down

    return jax.shard_map(local_block, mesh=mesh, in_specs=(tok_spec, weight_spec, weight_spec, weight_spec, P(None, None), P("dp"), tok_spec, tok_spec), out_specs=(tok_spec, slot_spec, slot_spec, slot_spec), check_vma=False)
```

```python
import functools

import jax
import jax.numpy as jnp
from jax import lax
from jax.experimental import pallas as pl
from jax.experimental.pallas import tpu as pltpu
from jax.sharding import PartitionSpec as P

ROUTE_SCALE = 2.5
LANES = 128
CORES = 2
MESH = pl.DeviceIdType.MESH


def block_kernel(groups, members, tok_ref, router_ref, table_ref, gate_ref, up_ref, down_ref,
                 y_ref, p_gate_ref, p_up_ref, p_down_ref,
                 toks, gates_all, ups_all, downs_all, piece_gate, piece_up, piece_down,
                 send_gate, send_up, send_down, sums, sums_in, tables, tables_s,
                 load_sem, swap_send, swap_recv, table_send, table_recv,
                 ring_send, ring_recv, sum_send, sum_recv, slot_send, slot_recv, slot_own, ):
    dp = lax.axis_index("dp")
    ep = lax.axis_index("ep")
    chips = members // CORES
    far = chips // 2
    plane = groups * CORES
    z = ep // CORES
    core = lax.rem(ep, CORES)
    q = dp * CORES + core
    above = (dp, lax.rem(z + 1, chips) * CORES + core)
    below = (dp, lax.rem(z + chips - 1, chips) * CORES + core)
    partner = (dp, z * CORES + 1 - core)
    toward = (above, below)
    rows = toks.shape[1]
    half = rows // 2
    width = router_ref.shape[0]
    local = gate_ref.shape[0]
    owned = local * CORES
    slots = p_gate_ref.shape[0]

    def plane_device(k):
        other = lax.rem(q + k, plane)
        return (other // CORES, z * CORES + lax.rem(other, CORES))

    barrier = pltpu.get_barrier_semaphore()
    for device in toward:
        pl.semaphore_signal(barrier, inc=1, device_id=device, device_id_type=MESH)

    def greet(k, _):
        pl.semaphore_signal(barrier, inc=1, device_id=plane_device(k), device_id_type=MESH)
        return 0

    lax.fori_loop(1, plane, greet, 0)
    pl.semaphore_wait(barrier, plane + 1)

    def send(src, dst, send_sem, recv_sem, device):
        copy = pltpu.make_async_remote_copy(src_ref=src, dst_ref=dst, send_sem=send_sem, recv_sem=recv_sem, device_id=device, device_id_type=MESH)
        copy.start()
        return copy

    sent = []

    loads = [pltpu.make_async_copy(tok_ref, toks.at[0], load_sem.at[0])]
    mine = pl.ds(core * local, local)
    swaps = []
    ring = {}
    for d in range(2):
        ring[0, d, 1] = send(tok_ref, toks.at[2 + d], ring_send.at[0, d, 0], ring_recv.at[0, d, 0], toward[d])
    for i, (src, dst) in enumerate(((gate_ref, gates_all), (up_ref, ups_all), (down_ref, downs_all))):
        loads.append(pltpu.make_async_copy(src, dst.at[mine], load_sem.at[1 + i]))
        swaps.append(send(src, dst.at[mine], swap_send.at[i], swap_recv.at[i], partner))
    for load in loads:
        load.start()
    for k in range(1, groups):
        other = lax.rem(dp + k, groups)
        sent.append(send(table_ref, tables.at[dp], table_send.at[k], table_recv.at[k], (other, ep)))
    tables_own = pltpu.make_async_copy(table_ref, tables.at[dp], load_sem.at[4])
    tables_own.start()

    full = (None, gates_all, ups_all, downs_all)
    pieces = (None, piece_gate, piece_up, piece_down)

    def block_of(hop, d, lo=0, count=None):
        origin = lax.rem(z + chips - hop if d == 0 else z + hop, chips)
        return pl.ds(origin * owned + lo, owned if count is None else count)

    def start_piece(i):
        piece = pieces[i].shape[1]
        part = pl.ds(pl.multiple_of(q * piece, piece), piece)
        for d in range(2):
            ring[i, d, 1] = send(full[i].at[:, part, :], pieces[i].at[block_of(0, d)], ring_send.at[i, d, 0], ring_recv.at[i, d, 0], toward[d])
        pieces[i][block_of(0, 0)] = full[i][:, part, :]

    def forward(i, hop):
        for d in range(2):
            ring[i, d, hop - 1].wait_recv()
            if i == 0:
                have, goal = toks.at[2 * (hop - 1) + d], toks.at[2 * hop + d]
                if hop == far:
                    part = pl.ds(d * half, half)
                    have, goal = toks.at[2 * (hop - 1) + d, part], toks.at[1, part]
            else:
                where = block_of(hop - 1, d)
                if hop == far:
                    where = block_of(hop - 1, d, d * (owned // 2), owned // 2)
                have, goal = pieces[i].at[where], pieces[i].at[where]
            ring[i, d, hop] = send(have, goal, ring_send.at[i, d, hop - 1], ring_recv.at[i, d, hop - 1], toward[d])

    def serve(pair):
        both = toks[2 * pair:2 * pair + 2].reshape(2 * rows, toks.shape[2])
        hid = both[:, :width]
        chosen = both[:, width:].astype(jnp.float32) > 0.5
        logits = jnp.dot(hid, router_ref[...], preferred_element_type=jnp.float32)
        gates = jnp.where(chosen, jax.nn.sigmoid(logits), 0.0)
        weights = ROUTE_SCALE * gates / jnp.sum(gates, axis=1, keepdims=True)
        lane = lax.broadcasted_iota(jnp.int32, weights.shape, 1)

        sums[2 * pair:2 * pair + 2] = jnp.zeros((2, rows, width), jnp.float32)

        def expert(e, _):
            hit = (lane == z * owned + e) & chosen
            weight = jnp.sum(jnp.where(hit, weights, 0.0), axis=1, keepdims=True)
            served = jnp.sum(jnp.where(hit, 1.0, 0.0), axis=1, keepdims=True) > 0.5
            act_a = jnp.dot(hid, gates_all[e], preferred_element_type=jnp.float32)
            act_b = jnp.dot(hid, ups_all[e], preferred_element_type=jnp.float32)
            hidden_act = (jax.nn.silu(act_a) * act_b).astype(jnp.bfloat16)
            expert_out = jnp.dot(hidden_act, downs_all[e], preferred_element_type=jnp.float32)
            contrib = jnp.where(served, weight * expert_out.astype(jnp.bfloat16).astype(jnp.float32), 0.0)
            sums[2 * pair:2 * pair + 2] += contrib.reshape(2, rows, width)
            return 0

        lax.fori_loop(0, owned, expert, 0)

    outs = (None, p_gate_ref, p_up_ref, p_down_ref)
    staged = (None, send_gate, send_up, send_down)

    def slot_copy(i, k):
        piece = pieces[i].shape[1]
        place = pl.ds(pl.multiple_of(q * piece, piece), piece)
        return pltpu.make_async_remote_copy(
            src_ref=staged[i].at[k], dst_ref=outs[i].at[:, place, :], send_sem=slot_send.at[i - 1, k], recv_sem=slot_recv.at[i - 1, k],
            device_id=plane_device(k), device_id_type=MESH)

    def slot_copy_own(i):
        piece = pieces[i].shape[1]
        place = pl.ds(pl.multiple_of(q * piece, piece), piece)
        return pltpu.make_async_copy(staged[i].at[0], outs[i].at[:, place, :], slot_own.at[i - 1])

    def exchange(i):
        def pick(k, _):
            group, member = plane_device(k)
            for s in range(slots):
                expert = tables_s[group, 0, member * slots + s]
                staged[i][k, s] = pieces[i][expert]
            return 0

        lax.fori_loop(0, plane, pick, 0)

        def start(k, _):
            slot_copy(i, k).start()
            return 0

        lax.fori_loop(1, plane, start, 0)
        slot_copy_own(i).start()

    def finish(i):
        def wait(k, _):
            slot_copy(i, k).wait()
            return 0

        lax.fori_loop(1, plane, wait, 0)
        slot_copy_own(i).wait()

    def arrived(i, load_index):
        loads[load_index].wait()
        swaps[i - 1].wait()

    arrived(1, 1)
    start_piece(1)
    for hop in range(2, far + 1):
        forward(0, hop)
        forward(1, hop)
        if hop == far:
            arrived(2, 2) if far == 2 else None
            start_piece(2)
            start_piece(3)
        if hop == 2 and far > 2:
            arrived(2, 2)
            arrived(3, 3)
        serve(hop - 1)
    for d in range(2):
        ring[0, d, far].wait_recv()
    loads[0].wait()
    serve(0)
    for copy in sent:
        copy.wait()
    tables_own.wait()
    tables_load = pltpu.make_async_copy(tables, tables_s, load_sem.at[5])
    tables_load.start()
    tables_load.wait()
    for d in range(2):
        ring[1, d, far].wait_recv()
    exchange(1)
    for hop in range(2, far + 1):
        forward(2, hop)
        forward(3, hop)

    sums_sent = []

    def part_of(h):
        return slice(h * half, (h + 1) * half)

    def sum_copy(d, k, h):
        index = 1 if k == far else 2 * k + 1 - d
        copy = send(sums.at[index, pl.ds(h * half, half)], sums_in.at[d, k - 1, pl.ds(h * half, half)],
                    sum_send.at[d, k - 1, h], sum_recv.at[d, k - 1, h], toward[d])
        sums_sent.append(copy)
        return copy

    pending = {}
    for k, h in ((far, 0), (far - 1, 1)):
        for d in range(2):
            pending[d, k, h ^ d] = sum_copy(d, k, h ^ d)
    for i in (2, 3):
        for d in range(2):
            ring[i, d, far].wait_recv()
        exchange(i)
    for k in range(far - 1, 0, -1):
        for h in (0, 1):
            if (k, h) == (far - 1, 1):
                continue
            order = h if k == far - 1 else 1 - h
            for d in range(2):
                part = order ^ d
                pending[d, k + 1, part].wait_recv()
                index = 2 * k + 1 - d
                sums[index, part_of(part)] += sums_in[d, k, part_of(part)]
            for d in range(2):
                pending[d, k, order ^ d] = sum_copy(d, k, order ^ d)
    for h in (1, 0):
        for d in range(2):
            pending[d, 1, h ^ d].wait_recv()
    y_ref[...] = (sums[0] + sums_in[0, 0] + sums_in[1, 0]).astype(jnp.bfloat16)

    for copy in sums_sent:
        copy.wait_send()
    for copy in ring.values():
        copy.wait_send()
    for i in (1, 2, 3):
        finish(i)


def run_block(groups, members, tokens, router, table, w_gate, w_up, w_down, per_dev):
    rows, ext_width = tokens.shape
    local, width, inter = w_gate.shape
    chips = members // CORES
    plane = groups * CORES
    owned = local * CORES
    experts = local * members
    far = chips // 2
    bf16 = w_gate.dtype
    gate_rows, down_rows = width // plane, inter // plane
    dma = pltpu.SemaphoreType.DMA
    anywhere = pl.BlockSpec(memory_space=pl.ANY)
    in_vmem = pl.BlockSpec(memory_space=pltpu.VMEM)
    return pl.pallas_call(
        functools.partial(block_kernel, groups, members),
        out_shape=[
            jax.ShapeDtypeStruct((rows, width), bf16),
            jax.ShapeDtypeStruct((per_dev, width, inter), bf16),
            jax.ShapeDtypeStruct((per_dev, width, inter), bf16),
            jax.ShapeDtypeStruct((per_dev, inter, width), bf16),
        ],
        in_specs=[anywhere, in_vmem, anywhere, anywhere, anywhere, anywhere],
        out_specs=[in_vmem, anywhere, anywhere, anywhere],
        scratch_shapes=[
            pltpu.VMEM((chips, rows, ext_width), bf16),
            pltpu.VMEM((owned, width, inter), bf16),
            pltpu.VMEM((owned, width, inter), bf16),
            pltpu.VMEM((owned, inter, width), bf16),
            pltpu.VMEM((experts, gate_rows, inter), bf16),
            pltpu.VMEM((experts, gate_rows, inter), bf16),
            pltpu.VMEM((experts, down_rows, width), bf16),
            pltpu.VMEM((plane, per_dev, gate_rows, inter), bf16),
            pltpu.VMEM((plane, per_dev, gate_rows, inter), bf16),
            pltpu.VMEM((plane, per_dev, down_rows, width), bf16),
            pltpu.VMEM((chips, rows, width), jnp.float32),
            pltpu.VMEM((2, far, rows, width), jnp.float32),
            pltpu.VMEM((groups, 8, LANES), jnp.int32),
            pltpu.SMEM((groups, 8, LANES), jnp.int32),
            dma((6,)), dma((3,)), dma((3,)), dma((groups,)), dma((groups,)),
            dma((4, 2, far)), dma((4, 2, far)), dma((2, far, 2)), dma((2, far, 2)),
            dma((3, plane)), dma((3, plane)), dma((3,)),
        ],
        compiler_params=pltpu.CompilerParams(collective_id=0, has_side_effects=True, vmem_limit_bytes=67043328),
        name="moe_block",
    )(tokens, router, table, w_gate, w_up, w_down)


def solution(mesh):
    members = mesh.shape["ep"]
    groups = mesh.shape["dp"]
    tok_spec = P(("dp", "ep"), None)
    weight_spec = P("ep", None, None)
    slot_spec = P(("dp", "ep"), None, None)

    def local_block(hid_rows, w_gate, w_up, w_down, w_router, slot_expert, topk_idx, topk_slot):
        width, experts = w_router.shape
        chosen = jnp.any(topk_idx[:, :, None] == jnp.arange(LANES)[None, None, :], axis=1).astype(hid_rows.dtype)
        tokens = jnp.concatenate([hid_rows, chosen], axis=1)
        router = jnp.pad(w_router, ((0, 0), (0, LANES - experts)))
        table = jnp.broadcast_to(jnp.pad(slot_expert, (0, LANES - slot_expert.shape[0]))[None, :], (8, LANES))
        y_rows, p_gate, p_up, p_down = run_block(groups, members, tokens, router, table, w_gate, w_up, w_down, slot_expert.shape[0] // members)
        return y_rows, p_gate, p_up, p_down

    return jax.shard_map(local_block, mesh=mesh, in_specs=(tok_spec, weight_spec, weight_spec, weight_spec, P(None, None), P("dp"), tok_spec, tok_spec), out_specs=(tok_spec, slot_spec, slot_spec, slot_spec), check_vma=False)
```

```python
import functools

import jax
import jax.numpy as jnp
from jax import lax
from jax.experimental import pallas as pl
from jax.experimental.pallas import tpu as pltpu
from jax.sharding import PartitionSpec as P

ROUTE_SCALE = 2.5
LANES = 128
CORES = 2
MESH = pl.DeviceIdType.MESH


def block_kernel(groups, members, tok_ref, idx_ref, router_ref, table_ref, gate_ref, up_ref, down_ref,
                 y_ref, p_gate_ref, p_up_ref, p_down_ref,
                 toks, idxs, gates_all, ups_all, downs_all, piece_gate, piece_up, piece_down,
                 send_gate, send_up, send_down, sums, sums_in, tables, tables_s,
                 load_sem, swap_send, swap_recv, table_send, table_recv, tok_send, tok_recv,
                 ring_send, ring_recv, plane_send, plane_recv, pair_send, pair_recv,
                 sum_send, sum_recv, slot_send, slot_recv, slot_own):
    dp = lax.axis_index("dp")
    ep = lax.axis_index("ep")
    chips = members // CORES
    far = chips // 2
    plane = groups * CORES
    bits = [1 << b for b in range(groups.bit_length() - 1)]
    z = ep // CORES
    core = lax.rem(ep, CORES)
    q = dp * CORES + core
    above = (dp, lax.rem(z + 1, chips) * CORES + core)
    below = (dp, lax.rem(z + chips - 1, chips) * CORES + core)
    partner = (dp, z * CORES + 1 - core)
    toward = (above, below)
    rows, width = toks.shape[1:]
    half = rows // 2
    local = gate_ref.shape[0]
    owned = local * CORES
    slots = p_gate_ref.shape[0]

    def plane_device(k):
        other = lax.rem(q + k, plane)
        return (other // CORES, z * CORES + lax.rem(other, CORES))

    def other_group(r):
        group = dp
        for bit in bits:
            if r & bit:
                group = group + bit * (1 - 2 * lax.rem(dp // bit, 2))
        return group

    barrier = pltpu.get_barrier_semaphore()
    for device in toward:
        pl.semaphore_signal(barrier, inc=1, device_id=device, device_id_type=MESH)

    def greet(k, _):
        pl.semaphore_signal(barrier, inc=1, device_id=plane_device(k), device_id_type=MESH)
        return 0

    lax.fori_loop(1, plane, greet, 0)
    pl.semaphore_wait(barrier, plane + 1)

    sent = []

    def send(src, dst, send_sem, recv_sem, device):
        copy = pltpu.make_async_remote_copy(src_ref=src, dst_ref=dst, send_sem=send_sem, recv_sem=recv_sem, device_id=device, device_id_type=MESH)
        copy.start()
        sent.append(copy)
        return copy

    full = (gates_all, ups_all, downs_all)
    pieces = (piece_gate, piece_up, piece_down)
    staged = (send_gate, send_up, send_down)
    outs = (p_gate_ref, p_up_ref, p_down_ref)
    mine = pl.ds(core * local, local)
    loads = [pltpu.make_async_copy(src, dst.at[mine], load_sem.at[i]) for i, (src, dst) in enumerate(zip((gate_ref, up_ref, down_ref), full))]
    loads.append(pltpu.make_async_copy(tok_ref, toks.at[0], load_sem.at[3]))
    loads.append(pltpu.make_async_copy(idx_ref, idxs.at[0], load_sem.at[4]))
    loads.append(pltpu.make_async_copy(table_ref, tables.at[dp], load_sem.at[5]))
    swaps = []
    ring, toked, planed, paired, summed = {}, {}, {}, {}, {}

    def start():
        for i, src in enumerate((gate_ref, up_ref, down_ref)):
            swaps.append(send(src, full[i].at[mine], swap_send.at[i], swap_recv.at[i], partner))
            loads[i].start()
        for load in loads[3:]:
            load.start()
        for k in range(1, groups):
            swaps.append(send(table_ref, tables.at[dp], table_send.at[k], table_recv.at[k], (lax.rem(dp + k, groups), ep)))

    def arrived(i):
        loads[i].wait()
        swaps[i].wait_recv()
        piece = pieces[i].shape[1]
        pieces[i][block_of(0, 0, 0, owned)] = full[i][:owned, pl.ds(pl.multiple_of(q * piece, piece), piece), :]

    def tokens(hop):
        for d in range(2):
            if hop == 1:
                toked[d, 1, 0] = send(tok_ref, toks.at[2 + d], tok_send.at[d, 0, 0], tok_recv.at[d, 0, 0], toward[d])
                toked[d, 1, 1] = send(idx_ref, idxs.at[2 + d], tok_send.at[d, 0, 1], tok_recv.at[d, 0, 1], toward[d])
            else:
                part = pl.ds(d * half, half)
                toked[d, 2, 0] = send(toks.at[2 + d, part], toks.at[1, part], tok_send.at[d, 1, 0], tok_recv.at[d, 1, 0], toward[d])
                toked[d, 2, 1] = send(idxs.at[2 + d, :, part], idxs.at[1, :, part], tok_send.at[d, 1, 1], tok_recv.at[d, 1, 1], toward[d])

    def tokens_near():
        for d in range(2):
            for a in range(2):
                toked[d, 1, a].wait_recv()

    def tokens_far():
        loads[3].wait()
        loads[4].wait()
        for d in range(2):
            for a in range(2):
                toked[d, 2, a].wait_recv()

    def block_of(hop, d, lo, count):
        origin = lax.rem(z + chips - hop if d == 0 else z + hop, chips)
        return pl.ds(origin * owned + lo, count)

    def pass_on(i, short, hop):
        piece = pieces[i].shape[1]
        for d in range(2):
            h = 1 - d if short else d
            where = block_of(hop - 1, d, h * local, local)
            src = pieces[i].at[where]
            if hop == 1:
                src = full[i].at[pl.ds(h * local, local), pl.ds(pl.multiple_of(q * piece, piece), piece), :]
            else:
                ring[i, d, h, hop - 1].wait_recv()
            ring[i, d, h, hop] = send(src, pieces[i].at[where], ring_send.at[i, d, h, hop - 1], ring_recv.at[i, d, h, hop - 1], toward[d])

    def rebuild(i, step):
        piece = pieces[i].shape[1]

        def region(h, r):
            at = (other_group(r) * CORES + core) * piece
            return (pl.ds(owned + h * local, local), pl.ds(pl.multiple_of(at, piece), piece), slice(None))

        for h in range(2):
            own = block_of(far, h, h * local, local)
            ways = bits if h == 0 else bits[::-1]
            seen, fresh = [0], [0]
            for bit in ways[:step]:
                fresh = [r | bit for r in seen]
                seen = seen + fresh
            if step == 0:
                ring[i, h, h, far].wait_recv()
                full[i][region(h, 0)] = pieces[i][own]
            for r in fresh:
                if r:
                    planed[i, h, r].wait_recv()
                src = full[i].at[region(h, r)] if r else pieces[i].at[own]
                paired[i, h, r] = send(src, full[i].at[region(h, r)], pair_send.at[i, h, r], pair_recv.at[i, h, r], partner)
            if step < len(ways):
                bit = ways[step]
                for r in seen:
                    src = full[i].at[region(h, r)] if r else pieces[i].at[own]
                    planed[i, h, r | bit] = send(src, full[i].at[region(h, r)], plane_send.at[i, h, r | bit], plane_recv.at[i, h, r | bit], (other_group(bit), ep))

    def rebuilt():
        for copy in paired.values():
            copy.wait_recv()

    def serve(pair, second):
        hid = toks[2 * pair:2 * pair + 2].reshape(2 * rows, width)
        idx = jnp.concatenate([idxs[2 * pair], idxs[2 * pair + 1]], axis=1)
        router = router_ref[...]
        logits = lax.dot_general(router, hid, (((1,), (1,)), ((), ())), preferred_element_type=jnp.float32)
        name = lax.broadcasted_iota(jnp.int32, logits.shape, 0)
        chosen = name == idx[0:1]
        for j in range(1, idx.shape[0]):
            chosen = chosen | (name == idx[j:j + 1])
        gates = jnp.where(chosen, jax.nn.sigmoid(logits), 0.0)
        weights = ROUTE_SCALE * gates / jnp.sum(gates, axis=0, keepdims=True)
        weights = jnp.where(chosen, weights, -1.0)
        weights = jnp.concatenate([weights, jnp.full((LANES - weights.shape[0], weights.shape[1]), -1.0, jnp.float32)], axis=0).T
        lane = lax.broadcasted_iota(jnp.int32, weights.shape, 1)
        first = lax.rem(z + far * second, chips) * owned
        if not second:
            sums[2 * pair:2 * pair + 2] = jnp.zeros((2, rows, width), jnp.float32)

        def expert(e, _):
            weight = jnp.sum(jnp.where(lane == first + e, weights, 0.0), axis=1, keepdims=True)
            at = e + owned * second
            act_a = jnp.dot(hid, gates_all[at], preferred_element_type=jnp.float32)
            act_b = jnp.dot(hid, ups_all[at], preferred_element_type=jnp.float32)
            hidden_act = (jax.nn.silu(act_a) * act_b).astype(jnp.bfloat16)
            expert_out = jnp.dot(hidden_act, downs_all[at], preferred_element_type=jnp.float32)
            contrib = jnp.where(weight < 0.0, 0.0, weight * expert_out.astype(jnp.bfloat16).astype(jnp.float32))
            sums[2 * pair:2 * pair + 2] += contrib.reshape(2, rows, width)
            return 0

        lax.fori_loop(0, owned, expert, 0)

    def slot_copy(i, k):
        piece = pieces[i].shape[1]
        place = pl.ds(pl.multiple_of(q * piece, piece), piece)
        return pltpu.make_async_remote_copy(
            src_ref=staged[i].at[k], dst_ref=outs[i].at[:, place, :], send_sem=slot_send.at[i, k], recv_sem=slot_recv.at[i, k],
            device_id=plane_device(k), device_id_type=MESH)

    def slot_copy_own(i):
        piece = pieces[i].shape[1]
        place = pl.ds(pl.multiple_of(q * piece, piece), piece)
        return pltpu.make_async_copy(staged[i].at[0], outs[i].at[:, place, :], slot_own.at[i])

    def tables_ready():
        loads[5].wait()
        for copy in swaps[3:]:
            copy.wait_recv()
        load = pltpu.make_async_copy(tables, tables_s, load_sem.at[6])
        load.start()
        load.wait()

    def exchange(i):
        for d in range(2):
            ring[i, d, 1 - d, far - 1].wait_recv()

        def pick(k, _):
            group, member = plane_device(k)
            for s in range(slots):
                staged[i][k, s] = pieces[i][tables_s[group, 0, member * slots + s]]
            return 0

        def begin(k, _):
            slot_copy(i, k).start()
            return 0

        lax.fori_loop(0, plane, pick, 0)
        lax.fori_loop(1, plane, begin, 0)
        slot_copy_own(i).start()

    def finish(i):
        def wait(k, _):
            slot_copy(i, k).wait()
            return 0

        lax.fori_loop(1, plane, wait, 0)
        slot_copy_own(i).wait()

    def part_of(h):
        return slice(h * half, (h + 1) * half)

    def sum_copy(d, k, h):
        index = 1 if k == 2 else 3 - d
        part = pl.ds(h * half, half)
        summed[d, k, h] = send(sums.at[index, part], sums_in.at[d, k - 1, part], sum_send.at[d, k - 1, h], sum_recv.at[d, k - 1, h], toward[d])

    def sums_far():
        for d in range(2):
            sum_copy(d, 2, 1 - d)

    def sums_near():
        for d in range(2):
            sum_copy(d, 1, d)

    def sums_joined():
        for d in range(2):
            summed[d, 2, 1 - d].wait_recv()
            sums[3 - d, part_of(1 - d)] += sums_in[d, 1, part_of(1 - d)]
        for d in range(2):
            sum_copy(d, 1, 1 - d)

    gate, up, down, long, short = 0, 1, 2, 0, 1
    last = len(bits)
    start()
    tokens(1)
    arrived(gate)
    pass_on(gate, long, 1)
    pass_on(gate, short, 1)
    pass_on(gate, long, 2)
    pass_on(gate, long, 3)
    pass_on(gate, short, 2)
    pass_on(gate, long, 4)
    pass_on(gate, short, 3)
    arrived(up)
    pass_on(up, long, 1)
    rebuild(gate, 0)
    arrived(down)
    pass_on(down, long, 1)
    tables_ready()
    exchange(gate)
    pass_on(up, long, 2)
    pass_on(down, long, 2)
    pass_on(up, long, 3)
    rebuild(gate, 1)
    pass_on(down, long, 3)
    pass_on(up, long, 4)
    pass_on(down, long, 4)
    rebuild(up, 0)
    pass_on(up, short, 1)
    tokens_near()
    serve(1, 0)
    rebuild(down, 0)
    tokens(2)
    rebuild(up, 1)
    pass_on(up, short, 2)
    rebuild(down, 1)
    pass_on(up, short, 3)
    pass_on(down, short, 1)
    for step in range(2, last + 1):
        rebuild(gate, step)
    exchange(up)
    pass_on(down, short, 2)
    pass_on(down, short, 3)
    for step in range(2, last + 1):
        rebuild(up, step)
    tokens_far()
    serve(0, 0)
    for step in range(2, last + 1):
        rebuild(down, step)
    rebuilt()
    serve(0, 1)
    sums_far()
    exchange(down)
    serve(1, 1)
    sums_near()
    sums_joined()
    for d in range(2):
        for h in range(2):
            summed[d, 1, h].wait_recv()
    y_ref[...] = (sums[0] + sums_in[0, 0] + sums_in[1, 0]).astype(jnp.bfloat16)
    for copy in sent:
        copy.wait_send()
    for i in range(3):
        finish(i)


def run_block(groups, members, tokens, idx, router, table, w_gate, w_up, w_down, per_dev):
    rows, width = tokens.shape
    local, _, inter = w_gate.shape
    chips = members // CORES
    far = chips // 2
    plane = groups * CORES
    owned = local * CORES
    experts = local * members
    bf16 = w_gate.dtype
    gate_rows, down_rows = width // plane, inter // plane
    dma = pltpu.SemaphoreType.DMA
    anywhere = pl.BlockSpec(memory_space=pl.ANY)
    in_vmem = pl.BlockSpec(memory_space=pltpu.VMEM)
    return pl.pallas_call(
        functools.partial(block_kernel, groups, members),
        out_shape=[
            jax.ShapeDtypeStruct((rows, width), bf16),
            jax.ShapeDtypeStruct((per_dev, width, inter), bf16),
            jax.ShapeDtypeStruct((per_dev, width, inter), bf16),
            jax.ShapeDtypeStruct((per_dev, inter, width), bf16),
        ],
        in_specs=[anywhere, anywhere, in_vmem, anywhere, anywhere, anywhere, anywhere],
        out_specs=[in_vmem, anywhere, anywhere, anywhere],
        scratch_shapes=[
            pltpu.VMEM((4, rows, width), bf16),
            pltpu.VMEM((4,) + idx.shape, jnp.int32),
            pltpu.VMEM((2 * owned, width, inter), bf16),
            pltpu.VMEM((2 * owned, width, inter), bf16),
            pltpu.VMEM((2 * owned, inter, width), bf16),
            pltpu.VMEM((experts, gate_rows, inter), bf16),
            pltpu.VMEM((experts, gate_rows, inter), bf16),
            pltpu.VMEM((experts, down_rows, width), bf16),
            pltpu.VMEM((plane, per_dev, gate_rows, inter), bf16),
            pltpu.VMEM((plane, per_dev, gate_rows, inter), bf16),
            pltpu.VMEM((plane, per_dev, down_rows, width), bf16),
            pltpu.VMEM((4, rows, width), jnp.float32),
            pltpu.VMEM((2, 2, rows, width), jnp.float32),
            pltpu.VMEM((groups, 8, LANES), jnp.int32),
            pltpu.SMEM((groups, 8, LANES), jnp.int32),
            dma((7,)), dma((3,)), dma((3,)), dma((groups,)), dma((groups,)), dma((2, 2, 2)), dma((2, 2, 2)),
            dma((3, 2, 2, far)), dma((3, 2, 2, far)), dma((3, 2, groups)), dma((3, 2, groups)), dma((3, 2, groups)), dma((3, 2, groups)),
            dma((2, 2, 2)), dma((2, 2, 2)), dma((3, plane)), dma((3, plane)), dma((3,)),
        ],
        compiler_params=pltpu.CompilerParams(collective_id=0, has_side_effects=True, vmem_limit_bytes=67043328),
        name="moe_block",
    )(tokens, idx, router, table, w_gate, w_up, w_down)


def solution(mesh):
    members = mesh.shape["ep"]
    groups = mesh.shape["dp"]
    tok_spec = P(("dp", "ep"), None)
    weight_spec = P("ep", None, None)
    slot_spec = P(("dp", "ep"), None, None)

    def local_block(hid_rows, w_gate, w_up, w_down, w_router, slot_expert, topk_idx, topk_slot):
        table = jnp.broadcast_to(jnp.pad(slot_expert, (0, LANES - slot_expert.shape[0]))[None, :], (8, LANES))
        y_rows, p_gate, p_up, p_down = run_block(groups, members, hid_rows, topk_idx.T, w_router.T, table, w_gate, w_up, w_down, slot_expert.shape[0] // members)
        return y_rows, p_gate, p_up, p_down

    return jax.shard_map(local_block, mesh=mesh, in_specs=(tok_spec, weight_spec, weight_spec, weight_spec, P(None, None), P("dp"), tok_spec, tok_spec), out_specs=(tok_spec, slot_spec, slot_spec, slot_spec), check_vma=False)
```

```python
import functools

import jax
import jax.numpy as jnp
from jax import lax
from jax.experimental import pallas as pl
from jax.experimental.pallas import tpu as pltpu
from jax.sharding import PartitionSpec as P

ROUTE_SCALE = 2.5
LANES = 128
CORES = 2
MESH = pl.DeviceIdType.MESH


def block_kernel(groups, members, tok_ref, idx_ref, router_ref, table_ref, gate_ref, up_ref, down_ref,
                 y_ref, p_gate_ref, p_up_ref, p_down_ref,
                 toks, idxs, gates_all, ups_all, downs_all, piece_gate, piece_up, piece_down,
                 send_gate, send_up, send_down, sums, sums_in, tables, tables_s,
                 load_sem, own_sem, early_send, early_recv, swap_send, swap_recv, table_send, table_recv, tok_send, tok_recv,
                 ring_send, ring_recv, plane_send, plane_recv, pair_send, pair_recv,
                 sum_send, sum_recv, slot_send, slot_recv, slot_own):
    dp = lax.axis_index("dp")
    ep = lax.axis_index("ep")
    chips = members // CORES
    far = chips // 2
    plane = groups * CORES
    bits = [1 << b for b in range(groups.bit_length() - 1)]
    z = ep // CORES
    core = lax.rem(ep, CORES)
    q = dp * CORES + core
    above = (dp, lax.rem(z + 1, chips) * CORES + core)
    below = (dp, lax.rem(z + chips - 1, chips) * CORES + core)
    partner = (dp, z * CORES + 1 - core)
    toward = (above, below)
    rows, width = toks.shape[1:]
    half = rows // 2
    local = gate_ref.shape[0]
    owned = local * CORES
    slots = p_gate_ref.shape[0]

    def plane_device(k):
        other = lax.rem(q + k, plane)
        return (other // CORES, z * CORES + lax.rem(other, CORES))

    def other_group(r):
        group = dp
        for bit in bits:
            if r & bit:
                group = group + bit * (1 - 2 * lax.rem(dp // bit, 2))
        return group

    barrier = pltpu.get_barrier_semaphore()
    for device in toward:
        pl.semaphore_signal(barrier, inc=1, device_id=device, device_id_type=MESH)

    def greet(k, _):
        pl.semaphore_signal(barrier, inc=1, device_id=plane_device(k), device_id_type=MESH)
        return 0

    lax.fori_loop(1, plane, greet, 0)
    pl.semaphore_wait(barrier, plane + 1)

    sent = []

    def send(src, dst, send_sem, recv_sem, device):
        copy = pltpu.make_async_remote_copy(src_ref=src, dst_ref=dst, send_sem=send_sem, recv_sem=recv_sem, device_id=device, device_id_type=MESH)
        copy.start()
        sent.append(copy)
        return copy

    full = (gates_all, ups_all, downs_all)
    pieces = (piece_gate, piece_up, piece_down)
    staged = (send_gate, send_up, send_down)
    outs = (p_gate_ref, p_up_ref, p_down_ref)
    mine = pl.ds(core * local, local)
    loads = [pltpu.make_async_copy(src, dst.at[mine], load_sem.at[i]) for i, (src, dst) in enumerate(zip((gate_ref, up_ref, down_ref), full))]
    loads.append(pltpu.make_async_copy(tok_ref, toks.at[0], load_sem.at[3]))
    loads.append(pltpu.make_async_copy(idx_ref, idxs.at[0], load_sem.at[4]))
    loads.append(pltpu.make_async_copy(table_ref, tables.at[dp], load_sem.at[5]))
    swaps = []
    owns, earlies = [], []
    ring, toked, planed, paired, summed = {}, {}, {}, {}, {}

    def start():
        for i, src in enumerate((gate_ref, up_ref, down_ref)):
            piece = pieces[i].shape[1]
            place = pieces[i].at[block_of(0, 0, core * local, local)]
            theirs = (q + 1 - 2 * core) * piece
            earlies.append(send(src.at[:, pl.ds(pl.multiple_of(theirs, piece), piece), :], place, early_send.at[i], early_recv.at[i], partner))
            owns.append(pltpu.make_async_copy(src.at[:, pl.ds(pl.multiple_of(q * piece, piece), piece), :], place, own_sem.at[i]))
            owns[i].start()
        for i, src in enumerate((gate_ref, up_ref, down_ref)):
            swaps.append(send(src, full[i].at[mine], swap_send.at[i], swap_recv.at[i], partner))
            loads[i].start()
        for load in loads[3:]:
            load.start()
        for k in range(1, groups):
            swaps.append(send(table_ref, tables.at[dp], table_send.at[k], table_recv.at[k], (lax.rem(dp + k, groups), ep)))

    def arrived(i):
        owns[i].wait()
        earlies[i].wait_recv()

    def experts_ready():
        for i in range(3):
            loads[i].wait()
            swaps[i].wait_recv()

    def tokens(hop):
        for d in range(2):
            if hop == 1:
                toked[d, 1, 0] = send(tok_ref, toks.at[2 + d], tok_send.at[d, 0, 0], tok_recv.at[d, 0, 0], toward[d])
                toked[d, 1, 1] = send(idx_ref, idxs.at[2 + d], tok_send.at[d, 0, 1], tok_recv.at[d, 0, 1], toward[d])
            else:
                part = pl.ds(d * half, half)
                toked[d, 2, 0] = send(toks.at[2 + d, part], toks.at[1, part], tok_send.at[d, 1, 0], tok_recv.at[d, 1, 0], toward[d])
                toked[d, 2, 1] = send(idxs.at[2 + d, :, part], idxs.at[1, :, part], tok_send.at[d, 1, 1], tok_recv.at[d, 1, 1], toward[d])

    def tokens_near():
        for d in range(2):
            for a in range(2):
                toked[d, 1, a].wait_recv()

    def tokens_far():
        loads[3].wait()
        loads[4].wait()
        for d in range(2):
            for a in range(2):
                toked[d, 2, a].wait_recv()

    def block_of(hop, d, lo, count):
        origin = lax.rem(z + chips - hop if d == 0 else z + hop, chips)
        return pl.ds(origin * owned + lo, count)

    def pass_on(i, short, hop, e):
        for d in range(2):
            h = 1 - d if short else d
            where = pieces[i].at[block_of(hop - 1, d, h * local + e, 1)]
            if hop > 1:
                ring[i, d, h, e, hop - 1].wait_recv()
            ring[i, d, h, e, hop] = send(where, where, ring_send.at[i, d, h, e, hop - 1], ring_recv.at[i, d, h, e, hop - 1], toward[d])

    def rebuild(i, step, e):
        piece = pieces[i].shape[1]

        def region(h, r):
            at = (other_group(r) * CORES + core) * piece
            return (pl.ds(owned + h * local + e, 1), pl.ds(pl.multiple_of(at, piece), piece), slice(None))

        for h in range(2):
            own = block_of(far, h, h * local + e, 1)
            ways = bits if h == 0 else bits[::-1]
            seen, fresh = [0], [0]
            for bit in ways[:step]:
                fresh = [r | bit for r in seen]
                seen = seen + fresh
            if step == 0:
                ring[i, h, h, e, far].wait_recv()
                full[i][region(h, 0)] = pieces[i][own]
            for r in fresh:
                if r:
                    planed[i, h, e, r].wait_recv()
                src = full[i].at[region(h, r)] if r else pieces[i].at[own]
                paired[i, h, e, r] = send(src, full[i].at[region(h, r)], pair_send.at[i, h, e, r], pair_recv.at[i, h, e, r], partner)
            if step < len(ways):
                bit = ways[step]
                for r in seen:
                    src = full[i].at[region(h, r)] if r else pieces[i].at[own]
                    planed[i, h, e, r | bit] = send(src, full[i].at[region(h, r)], plane_send.at[i, h, e, r | bit], plane_recv.at[i, h, e, r | bit], (other_group(bit), ep))

    def rebuilt():
        for copy in paired.values():
            copy.wait_recv()

    def serve(pair, second):
        hid = toks[2 * pair:2 * pair + 2].reshape(2 * rows, width)
        idx = jnp.concatenate([idxs[2 * pair], idxs[2 * pair + 1]], axis=1)
        router = router_ref[...]
        logits = lax.dot_general(router, hid, (((1,), (1,)), ((), ())), preferred_element_type=jnp.float32)
        name = lax.broadcasted_iota(jnp.int32, logits.shape, 0)
        chosen = name == idx[0:1]
        for j in range(1, idx.shape[0]):
            chosen = chosen | (name == idx[j:j + 1])
        gates = jnp.where(chosen, jax.nn.sigmoid(logits), 0.0)
        weights = ROUTE_SCALE * gates / jnp.sum(gates, axis=0, keepdims=True)
        weights = jnp.where(chosen, weights, -1.0)
        weights = jnp.concatenate([weights, jnp.full((LANES - weights.shape[0], weights.shape[1]), -1.0, jnp.float32)], axis=0).T
        lane = lax.broadcasted_iota(jnp.int32, weights.shape, 1)
        first = lax.rem(z + far * second, chips) * owned
        if not second:
            sums[2 * pair:2 * pair + 2] = jnp.zeros((2, rows, width), jnp.float32)

        def expert(e, _):
            weight = jnp.sum(jnp.where(lane == first + e, weights, 0.0), axis=1, keepdims=True)
            at = e + owned * second
            act_a = jnp.dot(hid, gates_all[at], preferred_element_type=jnp.float32)
            act_b = jnp.dot(hid, ups_all[at], preferred_element_type=jnp.float32)
            hidden_act = (jax.nn.silu(act_a) * act_b).astype(jnp.bfloat16)
            expert_out = jnp.dot(hidden_act, downs_all[at], preferred_element_type=jnp.float32)
            contrib = jnp.where(weight < 0.0, 0.0, weight * expert_out.astype(jnp.bfloat16).astype(jnp.float32))
            sums[2 * pair:2 * pair + 2] += contrib.reshape(2, rows, width)
            return 0

        lax.fori_loop(0, owned, expert, 0)

    def slot_copy(i, k):
        piece = pieces[i].shape[1]
        place = pl.ds(pl.multiple_of(q * piece, piece), piece)
        return pltpu.make_async_remote_copy(
            src_ref=staged[i].at[k], dst_ref=outs[i].at[:, place, :], send_sem=slot_send.at[i, k], recv_sem=slot_recv.at[i, k],
            device_id=plane_device(k), device_id_type=MESH)

    def slot_copy_own(i):
        piece = pieces[i].shape[1]
        place = pl.ds(pl.multiple_of(q * piece, piece), piece)
        return pltpu.make_async_copy(staged[i].at[0], outs[i].at[:, place, :], slot_own.at[i])

    def tables_ready():
        loads[5].wait()
        for copy in swaps[3:]:
            copy.wait_recv()
        load = pltpu.make_async_copy(tables, tables_s, load_sem.at[6])
        load.start()
        load.wait()

    def exchange(i):
        for d in range(2):
            for e in range(local):
                ring[i, d, 1 - d, e, far - 1].wait_recv()

        def pick(k, _):
            group, member = plane_device(k)
            for s in range(slots):
                staged[i][k, s] = pieces[i][tables_s[group, 0, member * slots + s]]
            return 0

        def begin(k, _):
            slot_copy(i, k).start()
            return 0

        lax.fori_loop(0, plane, pick, 0)
        lax.fori_loop(1, plane, begin, 0)
        slot_copy_own(i).start()

    def finish(i):
        def wait(k, _):
            slot_copy(i, k).wait()
            return 0

        lax.fori_loop(1, plane, wait, 0)
        slot_copy_own(i).wait()

    def part_of(h):
        return slice(h * half, (h + 1) * half)

    def sum_copy(d, k, h):
        index = 1 if k == 2 else 3 - d
        part = pl.ds(h * half, half)
        summed[d, k, h] = send(sums.at[index, part], sums_in.at[d, k - 1, part], sum_send.at[d, k - 1, h], sum_recv.at[d, k - 1, h], toward[d])

    def sums_far():
        for d in range(2):
            sum_copy(d, 2, 1 - d)

    def sums_near():
        for d in range(2):
            sum_copy(d, 1, d)

    def sums_joined():
        for d in range(2):
            summed[d, 2, 1 - d].wait_recv()
            sums[3 - d, part_of(1 - d)] += sums_in[d, 1, part_of(1 - d)]
        for d in range(2):
            sum_copy(d, 1, 1 - d)

    gate, up, down, long, short = 0, 1, 2, 0, 1
    last = len(bits)
    start()
    arrived(gate)
    pass_on(gate, long, 1, 0)
    pass_on(gate, long, 1, 1)
    pass_on(gate, long, 2, 0)
    pass_on(gate, long, 2, 1)
    pass_on(gate, short, 1, 0)
    pass_on(gate, long, 3, 1)
    pass_on(gate, long, 3, 0)
    pass_on(gate, short, 1, 1)
    pass_on(gate, long, 4, 1)
    pass_on(gate, long, 4, 0)
    pass_on(gate, short, 2, 1)
    rebuild(gate, 0, 1)
    pass_on(gate, short, 2, 0)
    rebuild(gate, 0, 0)
    pass_on(gate, short, 3, 1)
    rebuild(gate, 1, 1)
    pass_on(gate, short, 3, 0)
    rebuild(gate, 1, 0)
    arrived(down)
    pass_on(down, long, 1, 1)
    pass_on(down, long, 1, 0)
    arrived(up)
    pass_on(up, long, 1, 1)
    tables_ready()
    exchange(gate)
    pass_on(down, long, 2, 1)
    pass_on(up, long, 1, 0)
    pass_on(up, long, 2, 1)
    pass_on(up, long, 2, 0)
    pass_on(up, long, 3, 1)
    pass_on(up, long, 3, 0)
    pass_on(up, long, 4, 1)
    for step in range(2, last + 1):
        rebuild(gate, step, 1)
    pass_on(down, long, 2, 0)
    pass_on(up, long, 4, 0)
    pass_on(down, long, 3, 1)
    pass_on(down, long, 3, 0)
    rebuild(up, 0, 1)
    for step in range(2, last + 1):
        rebuild(gate, step, 0)
    rebuild(up, 0, 0)
    pass_on(up, short, 1, 0)
    pass_on(up, short, 1, 1)
    pass_on(down, long, 4, 0)
    rebuild(up, 1, 1)
    pass_on(up, short, 2, 0)
    pass_on(down, long, 4, 1)
    rebuild(down, 0, 0)
    pass_on(up, short, 2, 1)
    pass_on(up, short, 3, 0)
    rebuild(up, 1, 0)
    pass_on(up, short, 3, 1)
    rebuild(down, 0, 1)
    tokens(1)
    rebuild(down, 1, 0)
    rebuild(down, 1, 1)
    pass_on(down, short, 1, 1)
    for step in range(2, last + 1):
        rebuild(up, step, 0)
    exchange(up)
    for step in range(2, last + 1):
        rebuild(down, step, 0)
    pass_on(down, short, 1, 0)
    tokens_near()
    tokens(2)
    experts_ready()
    serve(1, 0)
    pass_on(down, short, 2, 0)
    for step in range(2, last + 1):
        rebuild(up, step, 1)
    for step in range(2, last + 1):
        rebuild(down, step, 1)
    pass_on(down, short, 2, 1)
    tokens_far()
    serve(0, 0)
    pass_on(down, short, 3, 0)
    pass_on(down, short, 3, 1)
    rebuilt()
    serve(0, 1)
    sums_far()
    exchange(down)
    serve(1, 1)
    sums_near()
    sums_joined()
    for d in range(2):
        for h in range(2):
            summed[d, 1, h].wait_recv()
    y_ref[...] = (sums[0] + sums_in[0, 0] + sums_in[1, 0]).astype(jnp.bfloat16)
    for copy in sent:
        copy.wait_send()
    for i in range(3):
        finish(i)


def run_block(groups, members, tokens, idx, router, table, w_gate, w_up, w_down, per_dev):
    rows, width = tokens.shape
    local, _, inter = w_gate.shape
    chips = members // CORES
    far = chips // 2
    plane = groups * CORES
    owned = local * CORES
    experts = local * members
    bf16 = w_gate.dtype
    gate_rows, down_rows = width // plane, inter // plane
    dma = pltpu.SemaphoreType.DMA
    anywhere = pl.BlockSpec(memory_space=pl.ANY)
    in_vmem = pl.BlockSpec(memory_space=pltpu.VMEM)
    return pl.pallas_call(
        functools.partial(block_kernel, groups, members),
        out_shape=[
            jax.ShapeDtypeStruct((rows, width), bf16),
            jax.ShapeDtypeStruct((per_dev, width, inter), bf16),
            jax.ShapeDtypeStruct((per_dev, width, inter), bf16),
            jax.ShapeDtypeStruct((per_dev, inter, width), bf16),
        ],
        in_specs=[anywhere, anywhere, in_vmem, anywhere, anywhere, anywhere, anywhere],
        out_specs=[in_vmem, anywhere, anywhere, anywhere],
        scratch_shapes=[
            pltpu.VMEM((4, rows, width), bf16),
            pltpu.VMEM((4,) + idx.shape, jnp.int32),
            pltpu.VMEM((2 * owned, width, inter), bf16),
            pltpu.VMEM((2 * owned, width, inter), bf16),
            pltpu.VMEM((2 * owned, inter, width), bf16),
            pltpu.VMEM((experts, gate_rows, inter), bf16),
            pltpu.VMEM((experts, gate_rows, inter), bf16),
            pltpu.VMEM((experts, down_rows, width), bf16),
            pltpu.VMEM((plane, per_dev, gate_rows, inter), bf16),
            pltpu.VMEM((plane, per_dev, gate_rows, inter), bf16),
            pltpu.VMEM((plane, per_dev, down_rows, width), bf16),
            pltpu.VMEM((4, rows, width), jnp.float32),
            pltpu.VMEM((2, 2, rows, width), jnp.float32),
            pltpu.VMEM((groups, 8, LANES), jnp.int32),
            pltpu.SMEM((groups, 8, LANES), jnp.int32),
            dma((7,)), dma((3,)), dma((3,)), dma((3,)), dma((3,)), dma((3,)), dma((groups,)), dma((groups,)), dma((2, 2, 2)), dma((2, 2, 2)),
            dma((3, 2, 2, local, far)), dma((3, 2, 2, local, far)),
            dma((3, 2, local, groups)), dma((3, 2, local, groups)), dma((3, 2, local, groups)), dma((3, 2, local, groups)),
            dma((2, 2, 2)), dma((2, 2, 2)), dma((3, plane)), dma((3, plane)), dma((3,)),
        ],
        compiler_params=pltpu.CompilerParams(collective_id=0, has_side_effects=True, vmem_limit_bytes=67043328),
        name="moe_block",
    )(tokens, idx, router, table, w_gate, w_up, w_down)


def solution(mesh):
    members = mesh.shape["ep"]
    groups = mesh.shape["dp"]
    tok_spec = P(("dp", "ep"), None)
    weight_spec = P("ep", None, None)
    slot_spec = P(("dp", "ep"), None, None)

    def local_block(hid_rows, w_gate, w_up, w_down, w_router, slot_expert, topk_idx, topk_slot):
        table = jnp.broadcast_to(jnp.pad(slot_expert, (0, LANES - slot_expert.shape[0]))[None, :], (8, LANES))
        y_rows, p_gate, p_up, p_down = run_block(groups, members, hid_rows, topk_idx.T, w_router.T, table, w_gate, w_up, w_down, slot_expert.shape[0] // members)
        return y_rows, p_gate, p_up, p_down

    return jax.shard_map(local_block, mesh=mesh, in_specs=(tok_spec, weight_spec, weight_spec, weight_spec, P(None, None), P("dp"), tok_spec, tok_spec), out_specs=(tok_spec, slot_spec, slot_spec, slot_spec), check_vma=False)
```

```python
import functools

import jax
import jax.numpy as jnp
from jax import lax
from jax.experimental import pallas as pl
from jax.experimental.pallas import tpu as pltpu
from jax.sharding import PartitionSpec as P

ROUTE_SCALE = 2.5
LANES = 128
CORES = 2
MESH = pl.DeviceIdType.MESH


def block_kernel(groups, members, tok_ref, idx_ref, router_ref, table_ref, gate_ref, up_ref, down_ref,
                 y_ref, p_gate_ref, p_up_ref, p_down_ref,
                 toks, idxs, gates_all, ups_all, downs_all, piece_gate, piece_up, piece_down,
                 send_gate, send_down, sums, sums_in, sums_mid, tables, tables_s,
                 load_sem, own_sem, early_send, early_recv, swap_send, swap_recv, table_send, table_recv, tok_send, tok_recv,
                 ring_send, ring_recv, plane_send, plane_recv, pair_send, pair_recv,
                 sum_send, sum_recv, slot_send, slot_recv, slot_own):
    dp = lax.axis_index("dp")
    ep = lax.axis_index("ep")
    chips = members // CORES
    far = chips // 2
    plane = groups * CORES
    bits = [1 << b for b in range(groups.bit_length() - 1)]
    z = ep // CORES
    core = lax.rem(ep, CORES)
    q = dp * CORES + core
    above = (dp, lax.rem(z + 1, chips) * CORES + core)
    below = (dp, lax.rem(z + chips - 1, chips) * CORES + core)
    partner = (dp, z * CORES + 1 - core)
    toward = (above, below)
    rows, width = toks.shape[1:]
    half = rows // 2
    local = gate_ref.shape[0]
    owned = local * CORES
    slots = p_gate_ref.shape[0]

    def plane_device(k):
        other = lax.rem(q + k, plane)
        return (other // CORES, z * CORES + lax.rem(other, CORES))

    def other_group(r):
        group = dp
        for bit in bits:
            if r & bit:
                group = group + bit * (1 - 2 * lax.rem(dp // bit, 2))
        return group

    barrier = pltpu.get_barrier_semaphore()
    for device in toward:
        pl.semaphore_signal(barrier, inc=1, device_id=device, device_id_type=MESH)

    def greet(k, _):
        pl.semaphore_signal(barrier, inc=1, device_id=plane_device(k), device_id_type=MESH)
        return 0

    lax.fori_loop(1, plane, greet, 0)
    pl.semaphore_wait(barrier, plane + 1)

    sent = []

    def send(src, dst, send_sem, recv_sem, device):
        copy = pltpu.make_async_remote_copy(src_ref=src, dst_ref=dst, send_sem=send_sem, recv_sem=recv_sem, device_id=device, device_id_type=MESH)
        copy.start()
        sent.append(copy)
        return copy

    full = (gates_all, ups_all, downs_all)
    pieces = (piece_gate, piece_up, piece_down)
    staged = (send_gate, send_gate, send_down)
    outs = (p_gate_ref, p_up_ref, p_down_ref)
    mine = pl.ds(core * local, local)
    loads = [pltpu.make_async_copy(src, dst.at[mine], load_sem.at[i]) for i, (src, dst) in enumerate(zip((gate_ref, up_ref, down_ref), full))]
    loads.append(pltpu.make_async_copy(tok_ref, toks.at[0], load_sem.at[3]))
    loads.append(pltpu.make_async_copy(idx_ref, idxs.at[0], load_sem.at[4]))
    loads.append(pltpu.make_async_copy(table_ref, tables.at[dp], load_sem.at[5]))
    swaps = []
    owns, earlies = [], []
    ring, toked, planed, paired, summed = {}, {}, {}, {}, {}

    def start():
        for i, src in enumerate((gate_ref, up_ref, down_ref)):
            piece = pieces[i].shape[1]
            place = pieces[i].at[block_of(0, 0, core * local, local)]
            theirs = (q + 1 - 2 * core) * piece
            earlies.append(send(src.at[:, pl.ds(pl.multiple_of(theirs, piece), piece), :], place, early_send.at[i], early_recv.at[i], partner))
            owns.append(pltpu.make_async_copy(src.at[:, pl.ds(pl.multiple_of(q * piece, piece), piece), :], place, own_sem.at[i]))
            owns[i].start()
        for i, src in enumerate((gate_ref, up_ref, down_ref)):
            swaps.append(send(src, full[i].at[mine], swap_send.at[i], swap_recv.at[i], partner))
            loads[i].start()
        for load in loads[3:]:
            load.start()
        for k in range(1, groups):
            swaps.append(send(table_ref, tables.at[dp], table_send.at[k], table_recv.at[k], (lax.rem(dp + k, groups), ep)))

    def arrived(i):
        owns[i].wait()
        earlies[i].wait_recv()

    def experts_ready():
        for i in range(3):
            loads[i].wait()
            swaps[i].wait_recv()

    def tokens(hop):
        for d in range(2):
            if hop == 1:
                toked[d, 1, 0] = send(tok_ref, toks.at[2 + d], tok_send.at[d, 0, 0], tok_recv.at[d, 0, 0], toward[d])
                toked[d, 1, 1] = send(idx_ref, idxs.at[2 + d], tok_send.at[d, 0, 1], tok_recv.at[d, 0, 1], toward[d])
            else:
                part = pl.ds(d * half, half)
                toked[d, 2, 0] = send(toks.at[2 + d, part], toks.at[1, part], tok_send.at[d, 1, 0], tok_recv.at[d, 1, 0], toward[d])
                toked[d, 2, 1] = send(idxs.at[2 + d, :, part], idxs.at[1, :, part], tok_send.at[d, 1, 1], tok_recv.at[d, 1, 1], toward[d])

    def tokens_near():
        for d in range(2):
            for a in range(2):
                toked[d, 1, a].wait_recv()

    def tokens_far():
        loads[3].wait()
        loads[4].wait()
        for d in range(2):
            for a in range(2):
                toked[d, 2, a].wait_recv()

    def block_of(hop, d, lo, count):
        origin = lax.rem(z + chips - hop if d == 0 else z + hop, chips)
        return pl.ds(origin * owned + lo, count)

    def pass_on(i, short, hop, e):
        for d in range(2):
            h = 1 - d if short else d
            where = pieces[i].at[block_of(hop - 1, d, h * local + e, 1)]
            if hop > 1:
                ring[i, d, h, e, hop - 1].wait_recv()
            ring[i, d, h, e, hop] = send(where, where, ring_send.at[i, d, h, e, hop - 1], ring_recv.at[i, d, h, e, hop - 1], toward[d])

    def rebuild(i, step, e):
        piece = pieces[i].shape[1]

        def region(h, r):
            at = (other_group(r) * CORES + core) * piece
            return (pl.ds(owned + h * local + e, 1), pl.ds(pl.multiple_of(at, piece), piece), slice(None))

        for h in range(2):
            own = block_of(far, h, h * local + e, 1)
            ways = bits if h == 0 else bits[::-1]
            seen, fresh = [0], [0]
            for bit in ways[:step]:
                fresh = [r | bit for r in seen]
                seen = seen + fresh
            if step == 0:
                ring[i, h, h, e, far].wait_recv()
                full[i][region(h, 0)] = pieces[i][own]
            for r in fresh:
                if r:
                    planed[i, h, e, r].wait_recv()
                src = full[i].at[region(h, r)] if r else pieces[i].at[own]
                paired[i, h, e, r] = send(src, full[i].at[region(h, r)], pair_send.at[i, h, e, r], pair_recv.at[i, h, e, r], partner)
            if step < len(ways):
                bit = ways[step]
                for r in seen:
                    src = full[i].at[region(h, r)] if r else pieces[i].at[own]
                    planed[i, h, e, r | bit] = send(src, full[i].at[region(h, r)], plane_send.at[i, h, e, r | bit], plane_recv.at[i, h, e, r | bit], (other_group(bit), ep))

    def rebuilt():
        for copy in paired.values():
            copy.wait_recv()

    def serve(pair, second):
        hid = toks[2 * pair:2 * pair + 2].reshape(2 * rows, width)
        idx = jnp.concatenate([idxs[2 * pair], idxs[2 * pair + 1]], axis=1)
        router = router_ref[...]
        logits = lax.dot_general(router, hid, (((1,), (1,)), ((), ())), preferred_element_type=jnp.float32)
        name = lax.broadcasted_iota(jnp.int32, logits.shape, 0)
        chosen = name == idx[0:1]
        for j in range(1, idx.shape[0]):
            chosen = chosen | (name == idx[j:j + 1])
        gates = jnp.where(chosen, jax.nn.sigmoid(logits), 0.0)
        weights = ROUTE_SCALE * gates / jnp.sum(gates, axis=0, keepdims=True)
        weights = jnp.where(chosen, weights, -1.0)
        weights = jnp.concatenate([weights, jnp.full((LANES - weights.shape[0], weights.shape[1]), -1.0, jnp.float32)], axis=0).T
        lane = lax.broadcasted_iota(jnp.int32, weights.shape, 1)
        first = lax.rem(z + far * second, chips) * owned
        if not second:
            sums[2 * pair:2 * pair + 2] = jnp.zeros((2, rows, width), jnp.float32)

        def expert(e, _):
            weight = jnp.sum(jnp.where(lane == first + e, weights, 0.0), axis=1, keepdims=True)
            at = e + owned * second
            act_a = jnp.dot(hid, gates_all[at], preferred_element_type=jnp.float32)
            act_b = jnp.dot(hid, ups_all[at], preferred_element_type=jnp.float32)
            hidden_act = (jax.nn.silu(act_a) * act_b).astype(jnp.bfloat16)
            expert_out = jnp.dot(hidden_act, downs_all[at], preferred_element_type=jnp.float32)
            contrib = jnp.where(weight < 0.0, 0.0, weight * expert_out.astype(jnp.bfloat16).astype(jnp.float32))
            sums[2 * pair:2 * pair + 2] += contrib.reshape(2, rows, width)
            return 0

        lax.fori_loop(0, owned, expert, 0)

    def slot_copy(i, k):
        piece = pieces[i].shape[1]
        place = pl.ds(pl.multiple_of(q * piece, piece), piece)
        return pltpu.make_async_remote_copy(
            src_ref=staged[i].at[k], dst_ref=outs[i].at[:, place, :], send_sem=slot_send.at[i, k], recv_sem=slot_recv.at[i, k],
            device_id=plane_device(k), device_id_type=MESH)

    def slot_copy_own(i):
        piece = pieces[i].shape[1]
        place = pl.ds(pl.multiple_of(q * piece, piece), piece)
        return pltpu.make_async_copy(staged[i].at[0], outs[i].at[:, place, :], slot_own.at[i])

    def tables_ready():
        loads[5].wait()
        for copy in swaps[3:]:
            copy.wait_recv()
        load = pltpu.make_async_copy(tables, tables_s, load_sem.at[6])
        load.start()
        load.wait()

    def exchange(i):
        for d in range(2):
            for e in range(local):
                ring[i, d, 1 - d, e, far - 1].wait_recv()

        def pick(k, _):
            group, member = plane_device(k)
            for s in range(slots):
                staged[i][k, s] = pieces[i][tables_s[group, 0, member * slots + s]]
            return 0

        def begin(k, _):
            slot_copy(i, k).start()
            return 0

        if i == 1:
            left(0)
        lax.fori_loop(0, plane, pick, 0)
        lax.fori_loop(1, plane, begin, 0)
        slot_copy_own(i).start()

    def left(i):
        def wait(k, _):
            slot_copy(i, k).wait_send()
            return 0

        lax.fori_loop(1, plane, wait, 0)
        slot_copy_own(i).wait()

    def landed(i):
        def wait(k, _):
            slot_copy(i, k).wait_recv()
            return 0

        lax.fori_loop(1, plane, wait, 0)

    def part_of(h):
        return slice(h * half, (h + 1) * half)

    def sum_copy(d, k, h):
        index = 1 if k == 2 else 3 - d
        part = pl.ds(h * half, half)
        summed[d, k, h] = send(sums.at[index, part], sums_mid.at[d] if k == 2 else sums_in.at[d, part], sum_send.at[d, k - 1, h], sum_recv.at[d, k - 1, h], toward[d])

    def sums_far():
        for d in range(2):
            sum_copy(d, 2, 1 - d)

    def sums_near():
        for d in range(2):
            sum_copy(d, 1, d)

    def sums_joined():
        for d in range(2):
            summed[d, 2, 1 - d].wait_recv()
            sums[3 - d, part_of(1 - d)] += sums_mid[d]
        for d in range(2):
            sum_copy(d, 1, 1 - d)

    gate, up, down, long, short = 0, 1, 2, 0, 1
    last = len(bits)
    start()
    arrived(gate)
    pass_on(gate, long, 1, 0)
    pass_on(gate, long, 1, 1)
    pass_on(gate, long, 2, 0)
    pass_on(gate, long, 2, 1)
    pass_on(gate, short, 1, 0)
    pass_on(gate, long, 3, 1)
    pass_on(gate, long, 3, 0)
    pass_on(gate, short, 1, 1)
    pass_on(gate, long, 4, 1)
    pass_on(gate, long, 4, 0)
    pass_on(gate, short, 2, 1)
    rebuild(gate, 0, 1)
    pass_on(gate, short, 2, 0)
    rebuild(gate, 0, 0)
    pass_on(gate, short, 3, 1)
    rebuild(gate, 1, 1)
    pass_on(gate, short, 3, 0)
    rebuild(gate, 1, 0)
    arrived(down)
    pass_on(down, long, 1, 1)
    pass_on(down, long, 1, 0)
    arrived(up)
    pass_on(up, long, 1, 1)
    tables_ready()
    exchange(gate)
    pass_on(down, long, 2, 1)
    pass_on(up, long, 1, 0)
    pass_on(up, long, 2, 1)
    pass_on(up, long, 2, 0)
    pass_on(up, long, 3, 1)
    pass_on(up, long, 3, 0)
    pass_on(up, long, 4, 1)
    for step in range(2, last + 1):
        rebuild(gate, step, 1)
    pass_on(down, long, 2, 0)
    pass_on(up, long, 4, 0)
    pass_on(down, long, 3, 1)
    pass_on(down, long, 3, 0)
    rebuild(up, 0, 1)
    for step in range(2, last + 1):
        rebuild(gate, step, 0)
    rebuild(up, 0, 0)
    pass_on(up, short, 1, 0)
    pass_on(up, short, 1, 1)
    pass_on(down, long, 4, 0)
    rebuild(up, 1, 1)
    pass_on(up, short, 2, 0)
    pass_on(down, long, 4, 1)
    rebuild(down, 0, 0)
    pass_on(up, short, 2, 1)
    pass_on(up, short, 3, 0)
    rebuild(up, 1, 0)
    pass_on(up, short, 3, 1)
    rebuild(down, 0, 1)
    tokens(1)
    rebuild(down, 1, 0)
    rebuild(down, 1, 1)
    pass_on(down, short, 1, 1)
    for step in range(2, last + 1):
        rebuild(up, step, 0)
    exchange(up)
    for step in range(2, last + 1):
        rebuild(down, step, 0)
    pass_on(down, short, 1, 0)
    tokens_near()
    tokens(2)
    experts_ready()
    serve(1, 0)
    pass_on(down, short, 2, 0)
    for step in range(2, last + 1):
        rebuild(up, step, 1)
    for step in range(2, last + 1):
        rebuild(down, step, 1)
    pass_on(down, short, 2, 1)
    tokens_far()
    serve(0, 0)
    pass_on(down, short, 3, 0)
    pass_on(down, short, 3, 1)
    rebuilt()
    serve(0, 1)
    sums_far()
    exchange(down)
    serve(1, 1)
    sums_near()
    sums_joined()
    for d in range(2):
        for h in range(2):
            summed[d, 1, h].wait_recv()
    y_ref[...] = (sums[0] + sums_in[0] + sums_in[1]).astype(jnp.bfloat16)
    for copy in sent:
        copy.wait_send()
    left(1)
    left(2)
    for i in range(3):
        landed(i)


def run_block(groups, members, tokens, idx, router, table, w_gate, w_up, w_down, per_dev):
    rows, width = tokens.shape
    local, _, inter = w_gate.shape
    chips = members // CORES
    far = chips // 2
    plane = groups * CORES
    owned = local * CORES
    experts = local * members
    bf16 = w_gate.dtype
    gate_rows, down_rows = width // plane, inter // plane
    dma = pltpu.SemaphoreType.DMA
    anywhere = pl.BlockSpec(memory_space=pl.ANY)
    in_vmem = pl.BlockSpec(memory_space=pltpu.VMEM)
    return pl.pallas_call(
        functools.partial(block_kernel, groups, members),
        out_shape=[
            pltpu.VMEM((rows, width), bf16),
            pltpu.VMEM((per_dev, width, inter), bf16),
            pltpu.VMEM((per_dev, width, inter), bf16),
            pltpu.VMEM((per_dev, inter, width), bf16),
        ],
        in_specs=[anywhere, anywhere, in_vmem, anywhere, anywhere, anywhere, anywhere],
        out_specs=[in_vmem] * 4,
        scratch_shapes=[
            pltpu.VMEM((4, rows, width), bf16),
            pltpu.VMEM((4,) + idx.shape, jnp.int32),
            pltpu.VMEM((2 * owned, width, inter), bf16),
            pltpu.VMEM((2 * owned, width, inter), bf16),
            pltpu.VMEM((2 * owned, inter, width), bf16),
            pltpu.VMEM((experts, gate_rows, inter), bf16),
            pltpu.VMEM((experts, gate_rows, inter), bf16),
            pltpu.VMEM((experts, down_rows, width), bf16),
            pltpu.VMEM((plane, per_dev, gate_rows, inter), bf16),
            pltpu.VMEM((plane, per_dev, down_rows, width), bf16),
            pltpu.VMEM((4, rows, width), jnp.float32),
            pltpu.VMEM((2, rows, width), jnp.float32),
            pltpu.VMEM((2, rows // 2, width), jnp.float32),
            pltpu.VMEM((groups, 8, LANES), jnp.int32),
            pltpu.SMEM((groups, 8, LANES), jnp.int32),
            dma((7,)), dma((3,)), dma((3,)), dma((3,)), dma((3,)), dma((3,)), dma((groups,)), dma((groups,)), dma((2, 2, 2)), dma((2, 2, 2)),
            dma((3, 2, 2, local, far)), dma((3, 2, 2, local, far)),
            dma((3, 2, local, groups)), dma((3, 2, local, groups)), dma((3, 2, local, groups)), dma((3, 2, local, groups)),
            dma((2, 2, 2)), dma((2, 2, 2)), dma((3, plane)), dma((3, plane)), dma((3,)),
        ],
        compiler_params=pltpu.CompilerParams(collective_id=0, has_side_effects=True, vmem_limit_bytes=54 * 2**20),
        name="moe_block",
    )(tokens, idx, router, table, w_gate, w_up, w_down)


def store_kernel(*refs):
    half = len(refs) // 2
    copies = [pltpu.make_async_copy(refs[i], refs[half + i], refs[-1].at[i]) for i in range(half)]
    for copy in copies:
        copy.start()
    for copy in copies:
        copy.wait()


def store_results(*results):
    results = [pltpu.with_memory_space_constraint(x, pltpu.VMEM) for x in results]
    return pl.pallas_call(
        store_kernel,
        out_shape=[jax.ShapeDtypeStruct(x.shape, x.dtype) for x in results],
        in_specs=[pl.BlockSpec(memory_space=pltpu.VMEM)] * len(results),
        out_specs=[pl.BlockSpec(memory_space=pl.ANY)] * len(results),
        scratch_shapes=[pltpu.SemaphoreType.DMA((len(results),))],
        compiler_params=pltpu.CompilerParams(vmem_limit_bytes=16 * 2**20),
        name="store_results",
    )(*results)


def solution(mesh):
    members = mesh.shape["ep"]
    groups = mesh.shape["dp"]
    tok_spec = P(("dp", "ep"), None)
    weight_spec = P("ep", None, None)
    slot_spec = P(("dp", "ep"), None, None)

    def local_block(hid_rows, w_gate, w_up, w_down, w_router, slot_expert, topk_idx, topk_slot):
        table = jnp.broadcast_to(jnp.pad(slot_expert, (0, LANES - slot_expert.shape[0]))[None, :], (8, LANES))
        y_rows, p_gate, p_up, p_down = run_block(groups, members, hid_rows, topk_idx.T, w_router.T, table, w_gate, w_up, w_down, slot_expert.shape[0] // members)
        return store_results(y_rows, p_gate, p_up, p_down)

    return jax.shard_map(local_block, mesh=mesh, in_specs=(tok_spec, weight_spec, weight_spec, weight_spec, P(None, None), P("dp"), tok_spec, tok_spec), out_specs=(tok_spec, slot_spec, slot_spec, slot_spec), check_vma=False)
```

```python
import functools

import jax
import jax.numpy as jnp
from jax import lax
from jax.experimental import pallas as pl
from jax.experimental.pallas import tpu as pltpu
from jax.sharding import PartitionSpec as P

ROUTE_SCALE = 2.5
LANES = 128
CORES = 2
MESH = pl.DeviceIdType.MESH


def block_kernel(groups, members, tok_ref, idx_ref, router_ref, table_ref, gate_ref, up_ref, down_ref,
                 y_ref, p_gate_ref, p_up_ref, p_down_ref,
                 toks, idxs, gates_all, ups_all, downs_all, piece_gate, piece_gate_b, piece_up, piece_down,
                 send_gate, send_down, sums, sums_in, sums_mid, tables, tables_s,
                 load_sem, own_sem, early_send, early_recv, swap_send, swap_recv, table_send, table_recv, tok_send, tok_recv,
                 ring_send, ring_recv, plane_send, plane_recv, pair_send, pair_recv,
                 sum_send, sum_recv, slot_send, slot_recv, slot_own):
    dp = lax.axis_index("dp")
    ep = lax.axis_index("ep")
    chips = members // CORES
    far = chips // 2
    plane = groups * CORES
    bits = [1 << b for b in range(groups.bit_length() - 1)]
    z = ep // CORES
    core = lax.rem(ep, CORES)
    q = dp * CORES + core
    above = (dp, lax.rem(z + 1, chips) * CORES + core)
    below = (dp, lax.rem(z + chips - 1, chips) * CORES + core)
    partner = (dp, z * CORES + 1 - core)
    toward = (above, below)
    rows, width = toks.shape[1:]
    half = rows // 2
    local = gate_ref.shape[0]
    owned = local * CORES
    slots = p_gate_ref.shape[0]

    def plane_device(k):
        other = lax.rem(q + k, plane)
        return (other // CORES, z * CORES + lax.rem(other, CORES))

    def other_group(r):
        group = dp
        for bit in bits:
            if r & bit:
                group = group + bit * (1 - 2 * lax.rem(dp // bit, 2))
        return group

    barrier = pltpu.get_barrier_semaphore()
    for device in toward:
        pl.semaphore_signal(barrier, inc=1, device_id=device, device_id_type=MESH)

    def greet(k, _):
        pl.semaphore_signal(barrier, inc=1, device_id=plane_device(k), device_id_type=MESH)
        return 0

    lax.fori_loop(1, plane, greet, 0)
    pl.semaphore_wait(barrier, plane + 1)

    sent = []

    def send(src, dst, send_sem, recv_sem, device):
        copy = pltpu.make_async_remote_copy(src_ref=src, dst_ref=dst, send_sem=send_sem, recv_sem=recv_sem, device_id=device, device_id_type=MESH)
        copy.start()
        sent.append(copy)
        return copy

    full = (gates_all, ups_all, downs_all)
    pieces = ((piece_gate, piece_gate_b), (piece_up,) * 2, (piece_down,) * 2)
    sizes = [weight.shape[1] // plane for weight in (gate_ref, up_ref, down_ref)]
    staged = (send_gate, send_gate, send_down)
    outs = (p_gate_ref, p_up_ref, p_down_ref)
    mine = pl.ds(core * local, local)
    loads = [pltpu.make_async_copy(src, dst.at[mine], load_sem.at[i]) for i, (src, dst) in enumerate(zip((gate_ref, up_ref, down_ref), full))]
    loads.append(pltpu.make_async_copy(tok_ref, toks.at[0], load_sem.at[3]))
    loads.append(pltpu.make_async_copy(idx_ref, idxs.at[0], load_sem.at[4]))
    loads.append(pltpu.make_async_copy(table_ref, tables.at[dp], load_sem.at[5]))
    swaps = []
    owns, earlies = [], []
    ring, toked, planed, paired, summed = {}, {}, {}, {}, {}

    def start():
        for n, (i, e, src) in enumerate(((0, 0, gate_ref), (0, 1, gate_ref), (1, 0, up_ref), (2, 0, down_ref))):
            lo, part = rows_of(i, e)
            place = pieces[i][e].at[block_of(0, 0, core * local, local)]
            theirs, ours = ((p * sizes[i] + lo) for p in (q + 1 - 2 * core, q))
            earlies.append(send(src.at[:, pl.ds(pl.multiple_of(theirs, part), part), :], place, early_send.at[n], early_recv.at[n], partner))
            owns.append(pltpu.make_async_copy(src.at[:, pl.ds(pl.multiple_of(ours, part), part), :], place, own_sem.at[n]))
            owns[n].start()
        for i, src in enumerate((gate_ref, up_ref, down_ref)):
            swaps.append(send(src, full[i].at[mine], swap_send.at[i], swap_recv.at[i], partner))
            loads[i].start()
        for load in loads[3:]:
            load.start()
        for k in range(1, groups):
            swaps.append(send(table_ref, tables.at[dp], table_send.at[k], table_recv.at[k], (lax.rem(dp + k, groups), ep)))

    def arrived(i):
        for n in (i + 1,) if i else (0, 1):
            owns[n].wait()
            earlies[n].wait_recv()

    def experts_ready():
        for i in range(3):
            loads[i].wait()
            swaps[i].wait_recv()

    def tokens_on(d, kind, h, srcs, at):
        part = pl.ds(h * half, half)
        toked[d, kind, 0] = send(srcs[0].at[part], toks.at[at, part], tok_send.at[d, kind, 0], tok_recv.at[d, kind, 0], toward[d])
        toked[d, kind, 1] = send(srcs[1].at[:, part], idxs.at[at, :, part], tok_send.at[d, kind, 1], tok_recv.at[d, kind, 1], toward[d])

    def tokens_first():
        for d in range(2):
            tokens_on(d, 0, d, (tok_ref, idx_ref), 2 + d)

    def tokens_second():
        for d in range(2):
            tokens_on(d, 1, 1 - d, (tok_ref, idx_ref), 2 + d)

    def tokens_third():
        tokens_here(0)
        for d in range(2):
            tokens_on(d, 2, d, (toks.at[2 + d], idxs.at[2 + d]), 1)

    def tokens_here(kind):
        for d in range(2):
            for a in range(2):
                toked[d, kind, a].wait_recv()

    def own_tokens():
        loads[3].wait()
        loads[4].wait()

    def block_of(hop, d, lo, count):
        origin = lax.rem(z + chips - hop if d == 0 else z + hop, chips)
        return pl.ds(origin * owned + lo, count)

    def share_of(i, hop, d, h, e):
        return block_of(hop, d, h * local + e, 1) if i else block_of(hop, d, h * local, local)

    def pass_on(i, short, hop, e):
        for d in range(2):
            h = 1 - d if short else d
            where = pieces[i][e].at[share_of(i, hop - 1, d, h, e)]
            if hop > 1:
                ring[i, d, h, e, hop - 1].wait_recv()
            ring[i, d, h, e, hop] = send(where, where, ring_send.at[i, d, h, e, hop - 1], ring_recv.at[i, d, h, e, hop - 1], toward[d])

    def rebuild(i, step, e):
        piece = sizes[i]

        def region(h, r):
            at = (other_group(r) * CORES + core) * piece
            if i:
                return (pl.ds(owned + h * local + e, 1), pl.ds(pl.multiple_of(at, piece), piece), slice(None))
            part = piece // local
            return (pl.ds(owned + h * local, local), pl.ds(pl.multiple_of(at + e * part, part), part), slice(None))

        for h in range(2):
            own = share_of(i, far, h, h, e)
            ways = bits if h == 0 else bits[::-1]
            seen, fresh = [0], [0]
            for bit in ways[:step]:
                fresh = [r | bit for r in seen]
                seen = seen + fresh
            if step == 0:
                ring[i, h, h, e, far].wait_recv()
                full[i][region(h, 0)] = pieces[i][e][own]
            for r in fresh:
                if r:
                    planed[i, h, e, r].wait_recv()
                src = full[i].at[region(h, r)] if r else pieces[i][e].at[own]
                paired[i, h, e, r] = send(src, full[i].at[region(h, r)], pair_send.at[i, h, e, r], pair_recv.at[i, h, e, r], partner)
            if step < len(ways):
                bit = ways[step]
                for r in seen:
                    src = full[i].at[region(h, r)] if r else pieces[i][e].at[own]
                    planed[i, h, e, r | bit] = send(src, full[i].at[region(h, r)], plane_send.at[i, h, e, r | bit], plane_recv.at[i, h, e, r | bit], (other_group(bit), ep))

    def rebuilt():
        for copy in paired.values():
            copy.wait_recv()

    def serve(first_block, blocks, second):
        these = slice(first_block, first_block + blocks)
        hid = toks[these].reshape(blocks * rows, width)
        idx = jnp.concatenate([idxs[first_block + b] for b in range(blocks)], axis=1) if blocks > 1 else idxs[first_block]
        router = router_ref[...]
        logits = lax.dot_general(router, hid, (((1,), (1,)), ((), ())), preferred_element_type=jnp.float32)
        name = lax.broadcasted_iota(jnp.int32, logits.shape, 0)
        chosen = name == idx[0:1]
        for j in range(1, idx.shape[0]):
            chosen = chosen | (name == idx[j:j + 1])
        gates = jnp.where(chosen, jax.nn.sigmoid(logits), 0.0)
        weights = ROUTE_SCALE * gates / jnp.sum(gates, axis=0, keepdims=True)
        weights = jnp.where(chosen, weights, -1.0)
        weights = jnp.concatenate([weights, jnp.full((LANES - weights.shape[0], weights.shape[1]), -1.0, jnp.float32)], axis=0).T
        lane = lax.broadcasted_iota(jnp.int32, weights.shape, 1)
        first = lax.rem(z + far * second, chips) * owned
        if not second:
            sums[these] = jnp.zeros((blocks, rows, width), jnp.float32)

        def expert(e, _):
            weight = jnp.sum(jnp.where(lane == first + e, weights, 0.0), axis=1, keepdims=True)
            at = e + owned * second
            act_a = jnp.dot(hid, gates_all[at], preferred_element_type=jnp.float32)
            act_b = jnp.dot(hid, ups_all[at], preferred_element_type=jnp.float32)
            hidden_act = (jax.nn.silu(act_a) * act_b).astype(jnp.bfloat16)
            expert_out = jnp.dot(hidden_act, downs_all[at], preferred_element_type=jnp.float32)
            contrib = jnp.where(weight < 0.0, 0.0, weight * expert_out.astype(jnp.bfloat16).astype(jnp.float32))
            sums[these] += contrib.reshape(blocks, rows, width)
            return 0

        lax.fori_loop(0, owned, expert, 0)

    def rows_of(i, e):
        part = sizes[i] // (1 if i else local)
        return e * part, part

    def slot_copy(i, e, k):
        lo, part = rows_of(i, e)
        place = pl.ds(pl.multiple_of(q * sizes[i] + lo, part), part)
        return pltpu.make_async_remote_copy(
            src_ref=staged[i].at[k, :, pl.ds(lo, part)], dst_ref=outs[i].at[:, place, :],
            send_sem=slot_send.at[3 * e + i, k], recv_sem=slot_recv.at[3 * e + i, k], device_id=plane_device(k), device_id_type=MESH)

    def slot_copy_own(i, e):
        lo, part = rows_of(i, e)
        place = pl.ds(pl.multiple_of(q * sizes[i] + lo, part), part)
        return pltpu.make_async_copy(staged[i].at[0, :, pl.ds(lo, part)], outs[i].at[:, place, :], slot_own.at[3 * e + i])

    def tables_ready():
        loads[5].wait()
        for copy in swaps[3:]:
            copy.wait_recv()
        load = pltpu.make_async_copy(tables, tables_s, load_sem.at[6])
        load.start()
        load.wait()

    def exchange(i, e):
        for d in range(2):
            for share in range(local) if i else (e,):
                ring[i, d, 1 - d, share, far - 1].wait_recv()
        lo, part = rows_of(i, e)

        def pick(k, _):
            group, member = plane_device(k)
            for s in range(slots):
                staged[i][k, s, lo:lo + part] = pieces[i][e][tables_s[group, 0, member * slots + s]]
            return 0

        def begin(k, _):
            slot_copy(i, e, k).start()
            return 0

        if i == 1:
            left(0, 0)
            left(0, 1)
        lax.fori_loop(0, plane, pick, 0)
        lax.fori_loop(1, plane, begin, 0)
        slot_copy_own(i, e).start()

    def left(i, e):
        def wait(k, _):
            slot_copy(i, e, k).wait_send()
            return 0

        lax.fori_loop(1, plane, wait, 0)
        slot_copy_own(i, e).wait()

    def landed(i, e):
        def wait(k, _):
            slot_copy(i, e, k).wait_recv()
            return 0

        lax.fori_loop(1, plane, wait, 0)

    def part_of(h):
        return slice(h * half, (h + 1) * half)

    def sum_copy(d, k, h):
        index = 1 if k == 2 else 3 - d
        part = pl.ds(h * half, half)
        summed[d, k, h] = send(sums.at[index, part], sums_mid.at[d] if k == 2 else sums_in.at[d, part], sum_send.at[d, k - 1, h], sum_recv.at[d, k - 1, h], toward[d])

    def sums_far():
        for d in range(2):
            sum_copy(d, 2, 1 - d)

    def sums_near():
        for d in range(2):
            sum_copy(d, 1, d)

    def sums_joined():
        for d in range(2):
            summed[d, 2, 1 - d].wait_recv()
            sums[3 - d, part_of(1 - d)] += sums_mid[d]
        for d in range(2):
            sum_copy(d, 1, 1 - d)

    gate, up, down, long, short = 0, 1, 2, 0, 1
    last = len(bits)
    start()
    arrived(gate)
    pass_on(gate, long, 1, 0)
    pass_on(gate, short, 1, 0)
    pass_on(gate, long, 2, 0)
    pass_on(gate, short, 2, 0)
    pass_on(gate, long, 3, 0)
    pass_on(gate, long, 1, 1)
    pass_on(gate, long, 4, 0)
    pass_on(gate, short, 3, 0)
    pass_on(gate, short, 1, 1)
    rebuild(gate, 0, 0)
    arrived(down)
    pass_on(down, long, 1, 1)
    tables_ready()
    exchange(gate, 0)
    pass_on(gate, long, 2, 1)
    pass_on(gate, short, 2, 1)
    pass_on(down, long, 2, 1)
    pass_on(gate, long, 3, 1)
    pass_on(gate, short, 3, 1)
    pass_on(gate, long, 4, 1)
    arrived(up)
    pass_on(up, long, 1, 0)
    rebuild(gate, 1, 0)
    pass_on(down, long, 3, 1)
    rebuild(gate, 0, 1)
    pass_on(down, long, 1, 0)
    exchange(gate, 1)
    pass_on(down, long, 4, 1)
    for step in range(2, last + 1):
        rebuild(gate, step, 0)
    pass_on(down, long, 2, 0)
    pass_on(up, long, 1, 1)
    pass_on(down, long, 3, 0)
    pass_on(up, long, 2, 0)
    pass_on(down, long, 4, 0)
    rebuild(down, 0, 1)
    pass_on(up, long, 2, 1)
    pass_on(up, long, 3, 0)
    rebuild(gate, 1, 1)
    rebuild(down, 0, 0)
    pass_on(up, long, 3, 1)
    pass_on(up, long, 4, 0)
    pass_on(up, short, 1, 1)
    rebuild(down, 1, 1)
    pass_on(up, long, 4, 1)
    pass_on(up, short, 1, 0)
    rebuild(up, 0, 0)
    pass_on(up, short, 2, 1)
    rebuild(down, 1, 0)
    rebuild(up, 0, 1)
    pass_on(up, short, 2, 0)
    rebuild(up, 1, 0)
    for step in range(2, last + 1):
        rebuild(down, step, 1)
    pass_on(up, short, 3, 1)
    pass_on(up, short, 3, 0)
    rebuild(up, 1, 1)
    pass_on(down, short, 1, 0)
    tokens_first()
    for step in range(2, last + 1):
        rebuild(gate, step, 1)
    tokens_second()
    exchange(up, 0)
    pass_on(down, short, 2, 0)
    experts_ready()
    own_tokens()
    serve(0, 1, 0)
    for step in range(2, last + 1):
        rebuild(down, step, 0)
    for step in range(2, last + 1):
        rebuild(up, step, 1)
    pass_on(down, short, 1, 1)
    tokens_third()
    tokens_here(1)
    serve(2, 2, 0)
    pass_on(down, short, 2, 1)
    pass_on(down, short, 3, 0)
    for step in range(2, last + 1):
        rebuild(up, step, 0)
    tokens_here(2)
    serve(1, 1, 0)
    pass_on(down, short, 3, 1)
    rebuilt()
    serve(1, 1, 1)
    sums_far()
    exchange(down, 0)
    serve(2, 2, 1)
    sums_near()
    sums_joined()
    serve(0, 1, 1)
    for d in range(2):
        for h in range(2):
            summed[d, 1, h].wait_recv()
    y_ref[...] = (sums[0] + sums_in[0] + sums_in[1]).astype(jnp.bfloat16)
    for copy in sent:
        copy.wait_send()
    left(1, 0)
    left(2, 0)
    for i, e in ((0, 0), (0, 1), (1, 0), (2, 0)):
        landed(i, e)


def run_block(groups, members, tokens, idx, router, table, w_gate, w_up, w_down, per_dev):
    rows, width = tokens.shape
    local, _, inter = w_gate.shape
    chips = members // CORES
    far = chips // 2
    plane = groups * CORES
    owned = local * CORES
    experts = local * members
    bf16 = w_gate.dtype
    gate_rows, down_rows = width // plane, inter // plane
    dma = pltpu.SemaphoreType.DMA
    anywhere = pl.BlockSpec(memory_space=pl.ANY)
    in_vmem = pl.BlockSpec(memory_space=pltpu.VMEM)
    return pl.pallas_call(
        functools.partial(block_kernel, groups, members),
        out_shape=[
            pltpu.VMEM((rows, width), bf16),
            pltpu.VMEM((per_dev, width, inter), bf16),
            pltpu.VMEM((per_dev, width, inter), bf16),
            pltpu.VMEM((per_dev, inter, width), bf16),
        ],
        in_specs=[anywhere, anywhere, in_vmem, anywhere, anywhere, anywhere, anywhere],
        out_specs=[in_vmem] * 4,
        scratch_shapes=[
            pltpu.VMEM((4, rows, width), bf16),
            pltpu.VMEM((4,) + idx.shape, jnp.int32),
            pltpu.VMEM((2 * owned, width, inter), bf16),
            pltpu.VMEM((2 * owned, width, inter), bf16),
            pltpu.VMEM((2 * owned, inter, width), bf16),
            pltpu.VMEM((experts, gate_rows // local, inter), bf16),
            pltpu.VMEM((experts, gate_rows // local, inter), bf16),
            pltpu.VMEM((experts, gate_rows, inter), bf16),
            pltpu.VMEM((experts, down_rows, width), bf16),
            pltpu.VMEM((plane, per_dev, gate_rows, inter), bf16),
            pltpu.VMEM((plane, per_dev, down_rows, width), bf16),
            pltpu.VMEM((4, rows, width), jnp.float32),
            pltpu.VMEM((2, rows, width), jnp.float32),
            pltpu.VMEM((2, rows // 2, width), jnp.float32),
            pltpu.VMEM((groups, 8, LANES), jnp.int32),
            pltpu.SMEM((groups, 8, LANES), jnp.int32),
            dma((7,)), dma((4,)), dma((4,)), dma((4,)), dma((3,)), dma((3,)), dma((groups,)), dma((groups,)), dma((2, 3, 2)), dma((2, 3, 2)),
            dma((3, 2, 2, local, far)), dma((3, 2, 2, local, far)),
            dma((3, 2, local, groups)), dma((3, 2, local, groups)), dma((3, 2, local, groups)), dma((3, 2, local, groups)),
            dma((2, 2, 2)), dma((2, 2, 2)), dma((4, plane)), dma((4, plane)), dma((4,)),
        ],
        compiler_params=pltpu.CompilerParams(collective_id=0, has_side_effects=True, vmem_limit_bytes=54 * 2**20),
        name="moe_block",
    )(tokens, idx, router, table, w_gate, w_up, w_down)


def store_kernel(*refs):
    half = len(refs) // 2
    copies = [pltpu.make_async_copy(refs[i], refs[half + i], refs[-1].at[i]) for i in range(half)]
    for copy in copies:
        copy.start()
    for copy in copies:
        copy.wait()


def store_results(*results):
    results = [pltpu.with_memory_space_constraint(x, pltpu.VMEM) for x in results]
    return pl.pallas_call(
        store_kernel,
        out_shape=[jax.ShapeDtypeStruct(x.shape, x.dtype) for x in results],
        in_specs=[pl.BlockSpec(memory_space=pltpu.VMEM)] * len(results),
        out_specs=[pl.BlockSpec(memory_space=pl.ANY)] * len(results),
        scratch_shapes=[pltpu.SemaphoreType.DMA((len(results),))],
        compiler_params=pltpu.CompilerParams(vmem_limit_bytes=16 * 2**20),
        name="store_results",
    )(*results)


def solution(mesh):
    members = mesh.shape["ep"]
    groups = mesh.shape["dp"]
    tok_spec = P(("dp", "ep"), None)
    weight_spec = P("ep", None, None)
    slot_spec = P(("dp", "ep"), None, None)

    def local_block(hid_rows, w_gate, w_up, w_down, w_router, slot_expert, topk_idx, topk_slot):
        table = jnp.broadcast_to(jnp.pad(slot_expert, (0, LANES - slot_expert.shape[0]))[None, :], (8, LANES))
        y_rows, p_gate, p_up, p_down = run_block(groups, members, hid_rows, topk_idx.T, w_router.T, table, w_gate, w_up, w_down, slot_expert.shape[0] // members)
        return store_results(y_rows, p_gate, p_up, p_down)

    return jax.shard_map(local_block, mesh=mesh, in_specs=(tok_spec, weight_spec, weight_spec, weight_spec, P(None, None), P("dp"), tok_spec, tok_spec), out_specs=(tok_spec, slot_spec, slot_spec, slot_spec), check_vma=False)
```

```python
import functools

import jax
import jax.numpy as jnp
from jax import lax
from jax.experimental import pallas as pl
from jax.experimental.pallas import tpu as pltpu
from jax.sharding import PartitionSpec as P

ROUTE_SCALE = 2.5
LANES = 128
CORES = 2
MESH = pl.DeviceIdType.MESH


def block_kernel(groups, members, tok_ref, idx_ref, router_ref, table_ref, gate_ref, up_ref, down_ref,
                 y_ref, p_gate_ref, p_up_ref, p_down_ref,
                 toks, idxs, gates_all, ups_all, downs_all, piece_gate, piece_gate_b, piece_up, piece_down,
                 send_gate, send_down, sums, sums_in, sums_mid, tables, tables_s,
                 load_sem, own_sem, early_send, early_recv, swap_send, swap_recv, table_send, table_recv, tok_send, tok_recv,
                 ring_send, ring_recv, plane_send, plane_recv, pair_send, pair_recv,
                 sum_send, sum_recv, slot_send, slot_recv, slot_own):
    dp = lax.axis_index("dp")
    ep = lax.axis_index("ep")
    chips = members // CORES
    far = chips // 2
    plane = groups * CORES
    bits = [1 << b for b in range(groups.bit_length() - 1)]
    z = ep // CORES
    core = lax.rem(ep, CORES)
    q = dp * CORES + core
    above = (dp, lax.rem(z + 1, chips) * CORES + core)
    below = (dp, lax.rem(z + chips - 1, chips) * CORES + core)
    partner = (dp, z * CORES + 1 - core)
    toward = (above, below)
    rows, width = toks.shape[1:]
    half = rows // 2
    local = gate_ref.shape[0]
    owned = local * CORES
    slots = p_gate_ref.shape[0]

    def plane_device(k):
        other = lax.rem(q + k, plane)
        return (other // CORES, z * CORES + lax.rem(other, CORES))

    def other_group(r):
        group = dp
        for bit in bits:
            if r & bit:
                group = group + bit * (1 - 2 * lax.rem(dp // bit, 2))
        return group

    barrier = pltpu.get_barrier_semaphore()
    for device in toward:
        pl.semaphore_signal(barrier, inc=1, device_id=device, device_id_type=MESH)

    def greet(k, _):
        pl.semaphore_signal(barrier, inc=1, device_id=plane_device(k), device_id_type=MESH)
        return 0

    lax.fori_loop(1, plane, greet, 0)
    pl.semaphore_wait(barrier, plane + 1)

    sent = []

    def send(src, dst, send_sem, recv_sem, device):
        copy = pltpu.make_async_remote_copy(src_ref=src, dst_ref=dst, send_sem=send_sem, recv_sem=recv_sem, device_id=device, device_id_type=MESH)
        copy.start()
        sent.append(copy)
        return copy

    full = (gates_all, ups_all, downs_all)
    pieces = ((piece_gate, piece_gate_b), (piece_up,) * 2, (piece_down,) * 2)
    sizes = [weight.shape[1] // plane for weight in (gate_ref, up_ref, down_ref)]
    staged = (send_gate, send_gate, send_down)
    outs = (p_gate_ref, p_up_ref, p_down_ref)
    mine = pl.ds(core * local, local)
    loads = [pltpu.make_async_copy(src, dst.at[mine], load_sem.at[i]) for i, (src, dst) in enumerate(zip((gate_ref, up_ref, down_ref), full))]
    loads.append(pltpu.make_async_copy(tok_ref, toks.at[0], load_sem.at[3]))
    loads.append(pltpu.make_async_copy(idx_ref, idxs.at[0], load_sem.at[4]))
    loads.append(pltpu.make_async_copy(table_ref, tables.at[dp], load_sem.at[5]))
    swaps = []
    owns, earlies = [], []
    ring, toked, planed, paired, summed = {}, {}, {}, {}, {}

    def start():
        for n, (i, e, src) in enumerate(((0, 0, gate_ref), (0, 1, gate_ref), (1, 0, up_ref), (2, 0, down_ref))):
            lo, part = rows_of(i, e)
            place = pieces[i][e].at[block_of(0, 0, core * local, local)]
            theirs, ours = ((p * sizes[i] + lo) for p in (q + 1 - 2 * core, q))
            earlies.append(send(src.at[:, pl.ds(pl.multiple_of(theirs, part), part), :], place, early_send.at[n], early_recv.at[n], partner))
            owns.append(pltpu.make_async_copy(src.at[:, pl.ds(pl.multiple_of(ours, part), part), :], place, own_sem.at[n]))
            owns[n].start()
        for i, src in enumerate((gate_ref, up_ref, down_ref)):
            swaps.append(send(src, full[i].at[mine], swap_send.at[i], swap_recv.at[i], partner))
            loads[i].start()
        for load in loads[3:]:
            load.start()
        for k in range(1, groups):
            swaps.append(send(table_ref, tables.at[dp], table_send.at[k], table_recv.at[k], (lax.rem(dp + k, groups), ep)))

    def arrived(i):
        for n in (i + 1,) if i else (0, 1):
            owns[n].wait()
            earlies[n].wait_recv()

    def experts_ready():
        for i in range(3):
            loads[i].wait()
            swaps[i].wait_recv()

    def tokens_on(d, kind, h, srcs, at):
        part = pl.ds(h * half, half)
        toked[d, kind, 0] = send(srcs[0].at[part], toks.at[at, part], tok_send.at[d, kind, 0], tok_recv.at[d, kind, 0], toward[d])
        toked[d, kind, 1] = send(srcs[1].at[:, part], idxs.at[at, :, part], tok_send.at[d, kind, 1], tok_recv.at[d, kind, 1], toward[d])

    def tokens_first():
        for d in range(2):
            tokens_on(d, 0, d, (tok_ref, idx_ref), 2 + d)

    def tokens_second():
        for d in range(2):
            tokens_on(d, 1, 1 - d, (tok_ref, idx_ref), 2 + d)

    def tokens_third():
        tokens_here(0)
        for d in range(2):
            tokens_on(d, 2, d, (toks.at[2 + d], idxs.at[2 + d]), 1)

    def tokens_here(kind):
        for d in range(2):
            for a in range(2):
                toked[d, kind, a].wait_recv()

    def own_tokens():
        loads[3].wait()
        loads[4].wait()

    def block_of(hop, d, lo, count):
        origin = lax.rem(z + chips - hop if d == 0 else z + hop, chips)
        return pl.ds(origin * owned + lo, count)

    def share_of(i, hop, d, h, e):
        return block_of(hop, d, h * local + e, 1) if i else block_of(hop, d, h * local, local)

    def pass_on(i, short, hop, e):
        for d in range(2):
            h = 1 - d if short else d
            where = pieces[i][e].at[share_of(i, hop - 1, d, h, e)]
            if hop > 1:
                ring[i, d, h, e, hop - 1].wait_recv()
            ring[i, d, h, e, hop] = send(where, where, ring_send.at[i, d, h, e, hop - 1], ring_recv.at[i, d, h, e, hop - 1], toward[d])

    def rebuild(i, step, e):
        piece = sizes[i]

        def region(h, r):
            at = (other_group(r) * CORES + core) * piece
            if i:
                return (pl.ds(owned + h * local + e, 1), pl.ds(pl.multiple_of(at, piece), piece), slice(None))
            part = piece // local
            return (pl.ds(owned + h * local, local), pl.ds(pl.multiple_of(at + e * part, part), part), slice(None))

        for h in range(2):
            own = share_of(i, far, h, h, e)
            ways = bits if h == 0 else bits[::-1]
            seen, fresh = [0], [0]
            for bit in ways[:step]:
                fresh = [r | bit for r in seen]
                seen = seen + fresh
            if step == 0:
                ring[i, h, h, e, far].wait_recv()
                full[i][region(h, 0)] = pieces[i][e][own]
            for r in fresh:
                if r:
                    planed[i, h, e, r].wait_recv()
                src = full[i].at[region(h, r)] if r else pieces[i][e].at[own]
                paired[i, h, e, r] = send(src, full[i].at[region(h, r)], pair_send.at[i, h, e, r], pair_recv.at[i, h, e, r], partner)
            if step < len(ways):
                bit = ways[step]
                for r in seen:
                    src = full[i].at[region(h, r)] if r else pieces[i][e].at[own]
                    planed[i, h, e, r | bit] = send(src, full[i].at[region(h, r)], plane_send.at[i, h, e, r | bit], plane_recv.at[i, h, e, r | bit], (other_group(bit), ep))

    def rebuilt():
        for copy in paired.values():
            copy.wait_recv()

    def serve(first_block, blocks, second):
        these = slice(first_block, first_block + blocks)
        hid = toks[these].reshape(blocks * rows, width)
        idx = jnp.concatenate([idxs[first_block + b] for b in range(blocks)], axis=1) if blocks > 1 else idxs[first_block]
        router = router_ref[...]
        logits = lax.dot_general(router, hid, (((1,), (1,)), ((), ())), preferred_element_type=jnp.float32)
        name = lax.broadcasted_iota(jnp.int32, logits.shape, 0)
        chosen = name == idx[0:1]
        for j in range(1, idx.shape[0]):
            chosen = chosen | (name == idx[j:j + 1])
        gates = jnp.where(chosen, jax.nn.sigmoid(logits), 0.0)
        weights = ROUTE_SCALE * gates / jnp.sum(gates, axis=0, keepdims=True)
        weights = jnp.where(chosen, weights, -1.0)
        weights = jnp.concatenate([weights, jnp.full((LANES - weights.shape[0], weights.shape[1]), -1.0, jnp.float32)], axis=0).T
        lane = lax.broadcasted_iota(jnp.int32, weights.shape, 1)
        first = lax.rem(z + far * second, chips) * owned
        if not second:
            sums[these] = jnp.zeros((blocks, rows, width), jnp.float32)

        def expert(e, _):
            weight = jnp.sum(jnp.where(lane == first + e, weights, 0.0), axis=1, keepdims=True)
            at = e + owned * second
            act_a = jnp.dot(hid, gates_all[at], preferred_element_type=jnp.float32)
            act_b = jnp.dot(hid, ups_all[at], preferred_element_type=jnp.float32)
            hidden_act = (jax.nn.silu(act_a) * act_b).astype(jnp.bfloat16)
            expert_out = jnp.dot(hidden_act, downs_all[at], preferred_element_type=jnp.float32)
            contrib = jnp.where(weight < 0.0, 0.0, weight * expert_out.astype(jnp.bfloat16).astype(jnp.float32))
            sums[these] += contrib.reshape(blocks, rows, width)
            return 0

        lax.fori_loop(0, owned, expert, 0)

    def rows_of(i, e):
        part = sizes[i] // (1 if i else local)
        return e * part, part

    def slot_copy(i, e, k):
        lo, part = rows_of(i, e)
        place = pl.ds(pl.multiple_of(q * sizes[i] + lo, part), part)
        return pltpu.make_async_remote_copy(
            src_ref=staged[i].at[k, :, pl.ds(lo, part)], dst_ref=outs[i].at[:, place, :],
            send_sem=slot_send.at[3 * e + i, k], recv_sem=slot_recv.at[3 * e + i, k], device_id=plane_device(k), device_id_type=MESH)

    def slot_copy_own(i, e):
        lo, part = rows_of(i, e)
        place = pl.ds(pl.multiple_of(q * sizes[i] + lo, part), part)
        return pltpu.make_async_copy(staged[i].at[0, :, pl.ds(lo, part)], outs[i].at[:, place, :], slot_own.at[3 * e + i])

    def tables_ready():
        loads[5].wait()
        for copy in swaps[3:]:
            copy.wait_recv()
        load = pltpu.make_async_copy(tables, tables_s, load_sem.at[6])
        load.start()
        load.wait()

    def exchange(i, e):
        for d in range(2):
            for share in range(local) if i else (e,):
                ring[i, d, 1 - d, share, far - 1].wait_recv()
        lo, part = rows_of(i, e)

        def pick(k, _):
            group, member = plane_device(k)
            for s in range(slots):
                staged[i][k, s, lo:lo + part] = pieces[i][e][tables_s[group, 0, member * slots + s]]
            return 0

        def begin(k, _):
            slot_copy(i, e, k).start()
            return 0

        if i == 1:
            left(0, 0)
            left(0, 1)
        lax.fori_loop(0, plane, pick, 0)
        lax.fori_loop(1, plane, begin, 0)
        slot_copy_own(i, e).start()

    def left(i, e):
        def wait(k, _):
            slot_copy(i, e, k).wait_send()
            return 0

        lax.fori_loop(1, plane, wait, 0)
        slot_copy_own(i, e).wait()

    def landed(i, e):
        def wait(k, _):
            slot_copy(i, e, k).wait_recv()
            return 0

        lax.fori_loop(1, plane, wait, 0)

    def part_of(h):
        return slice(h * half, (h + 1) * half)

    def sum_copy(d, k, h):
        index = 1 if k == 2 else 3 - d
        part = pl.ds(h * half, half)
        summed[d, k, h] = send(sums.at[index, part], sums_mid.at[d] if k == 2 else sums_in.at[d, part], sum_send.at[d, k - 1, h], sum_recv.at[d, k - 1, h], toward[d])

    def sums_far():
        for d in range(2):
            sum_copy(d, 2, 1 - d)

    def sums_near():
        for d in range(2):
            sum_copy(d, 1, d)

    def sums_joined():
        for d in range(2):
            summed[d, 2, 1 - d].wait_recv()
            sums[3 - d, part_of(1 - d)] += sums_mid[d]
        for d in range(2):
            sum_copy(d, 1, 1 - d)

    gate, up, down, long, short = 0, 1, 2, 0, 1
    last = len(bits)
    start()
    arrived(gate)
    pass_on(gate, long, 1, 0)
    pass_on(gate, short, 1, 0)
    pass_on(gate, long, 2, 0)
    pass_on(gate, short, 2, 0)
    pass_on(gate, long, 3, 0)
    pass_on(gate, long, 1, 1)
    pass_on(gate, long, 4, 0)
    pass_on(gate, short, 3, 0)
    pass_on(gate, short, 1, 1)
    rebuild(gate, 0, 0)
    arrived(down)
    pass_on(down, long, 1, 1)
    tables_ready()
    exchange(gate, 0)
    pass_on(gate, long, 2, 1)
    pass_on(gate, short, 2, 1)
    pass_on(down, long, 2, 1)
    pass_on(gate, long, 3, 1)
    pass_on(gate, short, 3, 1)
    pass_on(gate, long, 4, 1)
    arrived(up)
    pass_on(up, long, 1, 0)
    rebuild(gate, 1, 0)
    pass_on(down, long, 3, 1)
    rebuild(gate, 0, 1)
    pass_on(down, long, 1, 0)
    exchange(gate, 1)
    pass_on(down, long, 4, 1)
    for step in range(2, last + 1):
        rebuild(gate, step, 0)
    pass_on(down, long, 2, 0)
    pass_on(up, long, 1, 1)
    pass_on(down, long, 3, 0)
    pass_on(up, long, 2, 0)
    pass_on(down, long, 4, 0)
    rebuild(down, 0, 1)
    pass_on(up, long, 2, 1)
    pass_on(up, long, 3, 0)
    rebuild(gate, 1, 1)
    rebuild(down, 0, 0)
    pass_on(up, long, 3, 1)
    pass_on(up, long, 4, 0)
    pass_on(up, short, 1, 1)
    rebuild(down, 1, 1)
    pass_on(up, long, 4, 1)
    pass_on(up, short, 1, 0)
    rebuild(up, 0, 0)
    pass_on(up, short, 2, 1)
    rebuild(down, 1, 0)
    rebuild(up, 0, 1)
    pass_on(up, short, 2, 0)
    rebuild(up, 1, 0)
    for step in range(2, last + 1):
        rebuild(down, step, 1)
    pass_on(up, short, 3, 1)
    pass_on(up, short, 3, 0)
    rebuild(up, 1, 1)
    pass_on(down, short, 1, 0)
    tokens_first()
    for step in range(2, last + 1):
        rebuild(gate, step, 1)
    tokens_second()
    exchange(up, 0)
    pass_on(down, short, 2, 0)
    experts_ready()
    own_tokens()
    serve(0, 1, 0)
    for step in range(2, last + 1):
        rebuild(down, step, 0)
    for step in range(2, last + 1):
        rebuild(up, step, 1)
    pass_on(down, short, 1, 1)
    tokens_third()
    tokens_here(1)
    serve(2, 2, 0)
    pass_on(down, short, 2, 1)
    pass_on(down, short, 3, 0)
    for step in range(2, last + 1):
        rebuild(up, step, 0)
    tokens_here(2)
    serve(1, 1, 0)
    pass_on(down, short, 3, 1)
    rebuilt()
    serve(1, 1, 1)
    sums_far()
    exchange(down, 0)
    serve(2, 2, 1)
    sums_near()
    sums_joined()
    serve(0, 1, 1)
    for d in range(2):
        for h in range(2):
            summed[d, 1, h].wait_recv()
    y_ref[...] = (sums[0] + sums_in[0] + sums_in[1]).astype(jnp.bfloat16)
    for copy in sent:
        copy.wait_send()
    left(1, 0)
    left(2, 0)
    for i, e in ((0, 0), (0, 1), (1, 0), (2, 0)):
        landed(i, e)


def run_block(groups, members, tokens, idx, router, table, w_gate, w_up, w_down, per_dev):
    rows, width = tokens.shape
    local, _, inter = w_gate.shape
    chips = members // CORES
    far = chips // 2
    plane = groups * CORES
    owned = local * CORES
    experts = local * members
    bf16 = w_gate.dtype
    gate_rows, down_rows = width // plane, inter // plane
    dma = pltpu.SemaphoreType.DMA
    anywhere = pl.BlockSpec(memory_space=pl.ANY)
    in_vmem = pl.BlockSpec(memory_space=pltpu.VMEM)
    return pl.pallas_call(
        functools.partial(block_kernel, groups, members),
        out_shape=[
            pltpu.VMEM((rows, width), bf16),
            pltpu.VMEM((per_dev, width, inter), bf16),
            pltpu.VMEM((per_dev, width, inter), bf16),
            pltpu.VMEM((per_dev, inter, width), bf16),
        ],
        in_specs=[anywhere, anywhere, in_vmem, anywhere, anywhere, anywhere, anywhere],
        out_specs=[in_vmem] * 4,
        scratch_shapes=[
            pltpu.VMEM((4, rows, width), bf16),
            pltpu.VMEM((4,) + idx.shape, jnp.int32),
            pltpu.VMEM((2 * owned, width, inter), bf16),
            pltpu.VMEM((2 * owned, width, inter), bf16),
            pltpu.VMEM((2 * owned, inter, width), bf16),
            pltpu.VMEM((experts, gate_rows // local, inter), bf16),
            pltpu.VMEM((experts, gate_rows // local, inter), bf16),
            pltpu.VMEM((experts, gate_rows, inter), bf16),
            pltpu.VMEM((experts, down_rows, width), bf16),
            pltpu.VMEM((plane, per_dev, gate_rows, inter), bf16),
            pltpu.VMEM((plane, per_dev, down_rows, width), bf16),
            pltpu.VMEM((4, rows, width), jnp.float32),
            pltpu.VMEM((2, rows, width), jnp.float32),
            pltpu.VMEM((2, rows // 2, width), jnp.float32),
            pltpu.VMEM((groups, 8, LANES), jnp.int32),
            pltpu.SMEM((groups, 8, LANES), jnp.int32),
            dma((7,)), dma((4,)), dma((4,)), dma((4,)), dma((3,)), dma((3,)), dma((groups,)), dma((groups,)), dma((2, 3, 2)), dma((2, 3, 2)),
            dma((3, 2, 2, local, far)), dma((3, 2, 2, local, far)),
            dma((3, 2, local, groups)), dma((3, 2, local, groups)), dma((3, 2, local, groups)), dma((3, 2, local, groups)),
            dma((2, 2, 2)), dma((2, 2, 2)), dma((4, plane)), dma((4, plane)), dma((4,)),
        ],
        compiler_params=pltpu.CompilerParams(collective_id=0, has_side_effects=True, vmem_limit_bytes=54 * 2**20),
        name="moe_block",
    )(tokens, idx, router, table, w_gate, w_up, w_down)


def store_kernel(*refs):
    half = len(refs) // 2
    copies = [pltpu.make_async_copy(refs[i], refs[half + i], refs[-1].at[i]) for i in range(half)]
    for copy in copies:
        copy.start()
    for copy in copies:
        copy.wait()


def store_results(*results):
    results = [pltpu.with_memory_space_constraint(x, pltpu.VMEM) for x in results]
    return pl.pallas_call(
        store_kernel,
        out_shape=[jax.ShapeDtypeStruct(x.shape, x.dtype) for x in results],
        in_specs=[pl.BlockSpec(memory_space=pltpu.VMEM)] * len(results),
        out_specs=[pl.BlockSpec(memory_space=pl.ANY)] * len(results),
        scratch_shapes=[pltpu.SemaphoreType.DMA((len(results),))],
        compiler_params=pltpu.CompilerParams(vmem_limit_bytes=16 * 2**20),
        name="store_results",
    )(*results)


def solution(mesh):
    members = mesh.shape["ep"]
    groups = mesh.shape["dp"]
    tok_spec = P(("dp", "ep"), None)
    weight_spec = P("ep", None, None)
    slot_spec = P(("dp", "ep"), None, None)

    def local_block(hid_rows, w_gate, w_up, w_down, w_router, slot_expert, topk_idx, topk_slot):
        table = jnp.pad(slot_expert[None, :], ((0, 7), (0, LANES - slot_expert.shape[0])))
        y_rows, p_gate, p_up, p_down = run_block(groups, members, hid_rows, topk_idx.T, w_router.T, table, w_gate, w_up, w_down, slot_expert.shape[0] // members)
        return store_results(y_rows, p_gate, p_up, p_down)

    return jax.shard_map(local_block, mesh=mesh, in_specs=(tok_spec, weight_spec, weight_spec, weight_spec, P(None, None), P("dp"), tok_spec, tok_spec), out_specs=(tok_spec, slot_spec, slot_spec, slot_spec), check_vma=False)
```
